128 devices in a mesh: freq: 8 (over x, z_hi), space: 16 (over z_lo, y, core).
Axes of the slice: x: 4, y: 4, z: 4 (z_hi: 2, z_lo: 2; z = z_hi * 2 + z_lo), core: 2. Of those that a mesh axis runs over, the one named last changes fastest.
Arguments:
- spectra: bfloat16 [128, 49152, 256], P('freq', 'space'), may hold values from -48 to 48, as said below
- weight: float32 [49152], P('space'), may hold values from 0.25 to 4
- partner: int32 [128], P('freq'), may hold values from 0 to 15
- counts: int32 [128], P('freq'), may hold values from 1 to 8
Outputs:
- modes: bfloat16 [128, 16, 49152], P('freq', None, 'space')
- energy: float32 [128, 8], P('freq')
- coherence: float32 [128, 2, 8, 8], P('freq')
The draws below stay inside these ranges and needn't reach their ends.
Inputs may be any that keep to these rules, and one draw needn't show every extreme that they name: spectra are finite Fourier coefficients.
All inputs are finite; a program needn't handle non-finite values.
Results may differ from the reference program's by a relative error of at most 0.0045.
Values may be sent and summed in bfloat16 or wider, within the bound.
A program may use at most 128 MiB of HBM per device.

```python
import math
import jax
import jax.numpy as jnp
from jax import lax

NB = 128
FG = 16
KMAX = 8
ITERS = 4
NF = 128
NP = 49152
N_FREQ = 8


shared_terms = 256


def draw_spectra(key, part):
    keys = jax.random.split(key, 4)
    scales = jnp.exp(jax.random.uniform(keys[0], (NF, 1, NB), jnp.float32, 0.0, math.log(4.0)))
    noise = jax.random.normal(keys[1], (NF, NP, 2 * NB), jnp.float32)
    amplitude = 0.6
    shared = jax.random.normal(keys[2], (NP, shared_terms), jnp.float32)
    mixing = jax.random.normal(keys[3], (NF, shared_terms, 2 * NB), jnp.float32) * (amplitude * math.sqrt(8.0 / shared_terms))
    common = jnp.einsum('pr,frc->fpc', shared, mixing)
    doubled = jnp.concatenate([scales, scales], axis=2)
    return jnp.clip(doubled * (noise + common), -48.0, 48.0).astype(jnp.bfloat16)


def touch_ends(result, rng, low, high):
    place = [jax.random.randint(jax.random.fold_in(rng, axis), (), 0, length) for axis, length in enumerate(result.shape)]
    longest = result.shape.index(max(result.shape))
    beside = place[:longest] + [(place[longest] + 1) % result.shape[longest]] + place[longest + 1:]
    return result.at[tuple(place)].set(low).at[tuple(beside)].set(high)


def block_scale(rng, shape, cuts, smallest, high):
    loudness = 1.0
    for position, shards_of in cuts:
        heights = jax.random.uniform(jax.random.fold_in(jax.random.fold_in(rng, 6), position), (shards_of,), jnp.float32, smallest / len(cuts), high / len(cuts))
        loudness = loudness * jnp.repeat(jnp.exp(heights), shape[position] // shards_of).reshape((-1,) + (1,) * (len(shape) - 1 - position))
    return loudness


def setup_inputs(seed: int = 0) -> dict:
    arg_keys = jax.random.split(jax.random.key(seed), 5)
    return {
        "spectra": draw_spectra(jax.random.fold_in(arg_keys[4], 71), 0),
        "weight": jnp.clip(jnp.exp(math.log(4.0) - 2.7725887 * jax.random.uniform(arg_keys[1], (NP,), jnp.float32) ** block_scale(arg_keys[1], (NP,), ((0, 16),), -0.2, 0.2)), 0.25, 4.0),
        "partner": touch_ends(jax.random.randint(arg_keys[2], (NF,), 0, FG), jax.random.fold_in(arg_keys[2], 1), 0, FG - 1).astype(jnp.int32),
        "counts": touch_ends(jax.random.randint(arg_keys[3], (NF,), 1, KMAX + 1), jax.random.fold_in(arg_keys[3], 1), 1, KMAX).astype(jnp.int32),
    }


def embed(gram_re, gram_im):
    top = jnp.concatenate([gram_re, -gram_im], axis=2)
    bottom = jnp.concatenate([gram_im, gram_re], axis=2)
    return jnp.concatenate([top, bottom], axis=1)

def apply_operator(operator, basis):
    return jnp.einsum('fkc,fdc->fkd', basis, operator, precision=lax.Precision.HIGHEST)

def orthonormal(vectors, half):
    done = []
    for index in range(vectors.shape[1]):
        vector = vectors[:, index, :]
        for earlier in done:
            early_re, early_im = (earlier[:, :half], earlier[:, half:])
            vec_re, vec_im = (vector[:, :half], vector[:, half:])
            proj_re = lax.optimization_barrier(jnp.sum(early_re * vec_re + early_im * vec_im, axis=1, keepdims=True))
            proj_im = lax.optimization_barrier(jnp.sum(early_re * vec_im - early_im * vec_re, axis=1, keepdims=True))
            new_re = vec_re - proj_re * early_re + proj_im * early_im
            new_im = vec_im - proj_re * early_im - proj_im * early_re
            vector = jnp.concatenate([new_re, new_im], axis=1)
        length = jnp.sqrt(lax.optimization_barrier(jnp.sum(vector * vector, axis=1, keepdims=True)) + 1e-06)
        done.append(vector / length)
    return jnp.stack(done, axis=1)

def solve(gram_re, gram_im):
    half = gram_re.shape[1]
    operator = embed(gram_re, gram_im)
    basis = jnp.broadcast_to(jnp.eye(KMAX, 2 * half, dtype=jnp.float32), (gram_re.shape[0], KMAX, 2 * half))
    for sweep in range(ITERS):
        basis = orthonormal(apply_operator(operator, basis), half)
    image = apply_operator(operator, basis)
    energy = lax.optimization_barrier(jnp.sum(basis * image, axis=2))
    return (basis, energy)

def coefficients(basis, energy, counts):
    half = basis.shape[2] // 2
    ranks = jnp.arange(KMAX, dtype=jnp.int32)[None, :]
    scale = jnp.where(ranks < counts[:, None], 1.0 / jnp.sqrt(energy + 1e-06), 0.0)[:, :, None]
    part_re, part_im = (basis[:, :, :half], basis[:, :, half:])
    upper = jnp.concatenate([part_re, -part_im], axis=2) * scale
    lower = jnp.concatenate([part_im, part_re], axis=2) * scale
    return jnp.concatenate([upper, lower], axis=1).astype(jnp.bfloat16)

def reference(spectra, weight, partner, counts):
    half = NB

    def moment(block):
        weighted = (weight[:, None] * block).astype(jnp.bfloat16)
        return jnp.dot(block.T, weighted, preferred_element_type=jnp.float32)
    moments = lax.map(moment, spectra)
    gram_re = (moments[:, :half, :half] + moments[:, half:, half:]) / NP
    gram_im = (moments[:, :half, half:] - moments[:, half:, :half]) / NP
    basis, energy = solve(gram_re, gram_im)
    coefficient = coefficients(basis, energy, counts)

    def project(pair):
        return jnp.dot(pair[0], pair[1].T, preferred_element_type=jnp.float32).astype(jnp.bfloat16)
    modes = lax.map(project, (coefficient, spectra))
    freqs = jnp.arange(NF, dtype=jnp.int32)
    source = (N_FREQ - 1 - freqs // FG) * FG + partner
    partner_modes = jnp.take(modes, source.astype(jnp.int32), axis=0)

    def cohere(pair):
        phi = pair[0].astype(jnp.float32)
        psi = pair[1].astype(jnp.float32)
        wphi = phi * weight[None, :]
        hi = lax.Precision.HIGHEST
        real_part = jnp.dot(wphi[:KMAX], psi[:KMAX].T, precision=hi) + jnp.dot(wphi[KMAX:], psi[KMAX:].T, precision=hi)
        imag_part = jnp.dot(wphi[:KMAX], psi[KMAX:].T, precision=hi) - jnp.dot(wphi[KMAX:], psi[:KMAX].T, precision=hi)
        return jnp.stack([real_part, imag_part], axis=0) / NP
    coherence = lax.map(cohere, (modes, partner_modes))
    return (modes, energy, coherence)
```

```python
import functools

import jax
import jax.numpy as jnp
from jax import lax
from jax.experimental import pallas as pl
from jax.experimental.pallas import tpu as pltpu
from jax.sharding import PartitionSpec as P

KMAX = 8
ITERS = 4
EPS = 1e-06
AHEAD = 4
MESH = pl.DeviceIdType.MESH
HIGHEST = lax.Precision.HIGHEST


def moment(spectra, weighted):
    return lax.dot_general(
        spectra, weighted, (((0,), (0,)), ((), ())), preferred_element_type=jnp.float32
    )


def times_transposed(left, right):
    return lax.dot_general(
        left, right, (((1,), (1,)), ((), ())), preferred_element_type=jnp.float32
    )


def triangles(half):
    row = lax.broadcasted_iota(jnp.int32, (half, half), 0)
    col = lax.broadcasted_iota(jnp.int32, (half, half), 1)
    return row, col


def packed(moments):
    half = moments.shape[0] // 2
    row, col = triangles(half)
    gram_re = moments[:half, :half] + moments[half:, half:]
    gram_im = moments[:half, half:] - moments[half:, :half]
    return jnp.where(row <= col, gram_re, gram_im)


def unpacked(square, total):
    row, col = triangles(square.shape[0])
    flipped = square.T
    gram_re = jnp.where(row <= col, square, flipped)
    gram_im = jnp.where(row > col, square, jnp.where(row < col, -flipped, 0.0))
    return gram_re / total, gram_im / total


def orthonormal(vec_re, vec_im):
    ranks = lax.broadcasted_iota(jnp.int32, vec_re.shape, 0)
    for k in range(KMAX):
        own_re = jnp.broadcast_to(vec_re[k : k + 1], vec_re.shape)
        own_im = jnp.broadcast_to(vec_im[k : k + 1], vec_im.shape)
        norm = jnp.sum(own_re * own_re + own_im * own_im, axis=1, keepdims=True)
        proj_re = jnp.sum(own_re * vec_re + own_im * vec_im, axis=1, keepdims=True)
        proj_im = jnp.sum(own_re * vec_im - own_im * vec_re, axis=1, keepdims=True)
        inverse = 1.0 / jnp.sqrt(norm + EPS)
        unit_re, unit_im = own_re * inverse, own_im * inverse
        proj_re, proj_im = proj_re * inverse, proj_im * inverse
        new_re = vec_re - proj_re * unit_re + proj_im * unit_im
        new_im = vec_im - proj_re * unit_im - proj_im * unit_re
        vec_re = jnp.where(ranks > k, new_re, jnp.where(ranks == k, unit_re, vec_re))
        vec_im = jnp.where(ranks > k, new_im, jnp.where(ranks == k, unit_im, vec_im))
    return vec_re, vec_im


def solved(gram_re, gram_im, count):
    half = gram_re.shape[0]
    operator = jnp.concatenate([gram_re, gram_im], axis=1)

    def applied(vec_re, vec_im):
        both = jnp.concatenate([vec_re, vec_im], axis=0)
        image = jnp.dot(both, operator, precision=HIGHEST, preferred_element_type=jnp.float32)
        return (
            image[:KMAX, :half] + image[KMAX:, half:],
            image[KMAX:, :half] - image[:KMAX, half:],
        )

    vec_re, vec_im = orthonormal(gram_re[:KMAX], -gram_im[:KMAX])
    for _ in range(ITERS - 1):
        vec_re, vec_im = orthonormal(*applied(vec_re, vec_im))
    image_re, image_im = applied(vec_re, vec_im)
    energy = jnp.sum(vec_re * image_re + vec_im * image_im, axis=1, keepdims=True)
    ranks = lax.broadcasted_iota(jnp.int32, (KMAX, 1), 0)
    scale = jnp.where(ranks < count, 1.0 / jnp.sqrt(energy + EPS), 0.0)
    part_re, part_im = vec_re * scale, vec_im * scale
    coefficient = jnp.concatenate(
        [
            jnp.concatenate([part_re, -part_im], axis=1),
            jnp.concatenate([part_im, part_re], axis=1),
        ],
        axis=0,
    )
    return coefficient.astype(jnp.bfloat16), energy


def kernel(
    n_freq,
    n_space,
    total,
    spectra_hbm,
    weight_ref,
    partner_ref,
    counts_ref,
    modes_hbm,
    energy_ref,
    coherence_ref,
    spectra,
    column,
    weighted,
    squares,
    from_core,
    from_chips,
    coef_own,
    coefs,
    energy_own,
    energies,
    modes,
    arrived,
    weight_rows,
    weight_in,
    partner_row,
    partner_in,
    parts,
    parts_in,
    sums,
    load_sem,
    store_sem,
    core_send,
    core_recv,
    chip_send,
    chip_recv,
    coef_send,
    coef_recv,
    energy_send,
    energy_recv,
    mode_send,
    mode_recv,
    weight_sem,
    row_send,
    row_recv,
    part_send,
    part_recv,
    sum_send,
    sum_recv,
):
    freqs, points, wide = spectra.shape
    quarter = points // 4
    g, s = lax.axis_index("freq"), lax.axis_index("space")
    core, chip = lax.rem(s, 2), s // 2
    n_chips = n_space // 2
    n_y = max(n_chips // 2, 1)
    z_lo, y = chip // n_y, lax.rem(chip, n_y)
    x, z_hi = g // 2, lax.rem(g, 2)
    n_x = n_freq // 2

    def remote(src, dst, send, recv, device):
        return pltpu.make_async_remote_copy(
            src_ref=src,
            dst_ref=dst,
            send_sem=send,
            recv_sem=recv,
            device_id=device,
            device_id_type=MESH,
        )

    def space_peer(offset):
        return (g, lax.rem(s + offset, n_space))

    other_s = lax.rem(s + n_space // 2, n_space)

    def meeting(slot):
        to_x = x if slot < 2 else n_x - 1 - x
        to_z = z_hi if slot % 2 == 0 else 1 - z_hi
        part = 2 * to_z + (2 * to_x) // n_x
        return (2 * to_x + to_z, other_s), part

    def chip_at(step):
        ahead = n_chips - 1 - step
        to_z = lax.rem(z_lo + ahead // n_y, 2)
        to_y = lax.rem(y + lax.rem(ahead, n_y), n_y)
        return to_z * n_y + to_y

    def freq_at(step):
        first = step < n_chips
        place = jnp.where(first, step, step - n_chips)
        return 2 * chip_at(place) + jnp.where(first, 1 - core, core)

    def load(step):
        freq = freq_at(step)
        return pltpu.make_async_copy(spectra_hbm.at[freq], spectra.at[freq], load_sem.at[freq])

    for step in range(min(AHEAD, freqs)):
        load(step).start()

    barrier = pltpu.get_barrier_semaphore()
    for offset in range(1, n_space):
        pl.semaphore_signal(barrier, inc=1, device_id=space_peer(offset), device_id_type=MESH)
    for slot in range(1, 4):
        pl.semaphore_signal(barrier, inc=1, device_id=meeting(slot)[0], device_id_type=MESH)

    tiles = points // 128
    for tile in range(tiles):
        line = weight_ref[tile : tile + 1, :]
        column[tile * 128 : (tile + 1) * 128, :] = jnp.broadcast_to(line, (128, 128)).T
        place, within = tile // (tiles // 4), tile % (tiles // 4)
        weight_rows[place, :, within * 128 : (within + 1) * 128] = line
    lanes = partner_row.shape[1]
    which = lax.broadcasted_iota(jnp.int32, (1, lanes), 1) // (2 * KMAX)
    row = jnp.zeros((1, lanes), jnp.float32)
    for freq in range(freqs):
        row = jnp.where(which == freq, partner_ref[freq].astype(jnp.float32), row)
    partner_row[...] = row

    pl.semaphore_wait(barrier, n_space - 1 + 3)

    def core_copy(step):
        return remote(
            squares.at[step],
            from_core.at[step],
            core_send.at[step],
            core_recv.at[step],
            (g, s + 1 - 2 * core),
        )

    def chip_copy(step):
        return remote(
            squares.at[n_chips + step],
            from_chips.at[step],
            chip_send.at[step],
            chip_recv.at[step],
            (g, 2 * chip_at(step) + core),
        )

    def gram(step):
        freq = freq_at(step)
        load(step).wait()

        @pl.when(step + AHEAD < freqs)
        def _():
            load(step + AHEAD).start()

        rows = 256 if points % 256 == 0 else 128
        for start in range(0, points, rows):
            block = spectra[freq, start : start + rows, :].astype(jnp.float32)
            scale = column[start : start + rows, :]
            scale = jnp.concatenate([scale, scale], axis=1)
            weighted[start : start + rows, :] = (block * scale).astype(jnp.bfloat16)
        return packed(moment(spectra[freq], weighted[...]))

    @pl.loop(0, n_chips)
    def _(step):
        @pl.when(step >= 1)
        def _():
            core_copy(step - 1).start()

        squares[step] = gram(step)

    @pl.loop(0, n_chips)
    def _(step):
        @pl.when(step == 0)
        def _():
            core_copy(n_chips - 1).start()

        @pl.when(step >= 1)
        def _():
            chip_copy(step - 1).start()

        square = gram(n_chips + step)
        core_copy(step).wait_recv()
        squares[n_chips + step] = square + from_core[step]

    weight_copy = remote(
        weight_rows.at[meeting(0)[1]], weight_in, weight_sem.at[0], weight_sem.at[1], meeting(0)[0]
    )
    weight_copy.start()
    row_copies = [
        remote(
            partner_row, partner_in.at[slot], row_send.at[slot], row_recv.at[slot], meeting(slot)[0]
        )
        for slot in range(4)
    ]
    for copy in row_copies:
        copy.start()

    square = squares[2 * n_chips - 1]
    for step in range(n_chips - 1):
        chip_copy(step).wait_recv()
        square = square + from_chips[step]
    coefficient, energy = solved(*unpacked(square, total), counts_ref[s])
    coef_own[...] = coefficient
    energy_own[...] = jnp.broadcast_to(energy, energy_own.shape)
    coefs[s] = coefficient
    energies[s] = jnp.broadcast_to(energy, energy_own.shape)

    coef_copies, energy_copies, sum_copies = [], [], []
    for offset in range(1, n_space):
        peer = space_peer(offset)
        send, recv = coef_send.at[offset], coef_recv.at[offset]
        coef_copies.append(remote(coef_own, coefs.at[s], send, recv, peer))
        send, recv = energy_send.at[offset], energy_recv.at[offset]
        energy_copies.append(remote(energy_own, energies.at[s], send, recv, peer))
        send, recv = sum_send.at[offset], sum_recv.at[offset]
        sum_copies.append(remote(sums.at[s], sums.at[s], send, recv, peer))
    for copy in coef_copies:
        copy.start()
    for copy in energy_copies:
        copy.start()
    for copy in coef_copies:
        copy.wait_recv()

    def mode_copy(freq, slot):
        device, part = meeting(slot)
        start = pl.multiple_of(part * quarter, 128)
        return remote(
            modes.at[freq, :, pl.ds(start, quarter)],
            arrived.at[slot, freq],
            mode_send.at[slot, freq],
            mode_recv.at[slot, freq],
            device,
        )

    def mode_store(freq):
        return pltpu.make_async_copy(modes.at[freq], modes_hbm.at[freq], store_sem.at[freq])

    @pl.loop(0, freqs)
    def _(freq):
        modes[freq] = times_transposed(coefs[freq], spectra[freq]).astype(jnp.bfloat16)
        for slot in range(4):
            mode_copy(freq, slot).start()
        mode_store(freq).start()

    for copy in row_copies:
        copy.wait_recv()
    weight_copy.wait_recv()

    @pl.loop(0, freqs)
    def _(freq):
        for slot in range(4):
            mode_copy(freq, slot).wait_recv()

    rows = 2 * KMAX * freqs
    owner = lax.broadcasted_iota(jnp.int32, (rows, rows), 0) // (2 * KMAX)
    owner = owner.astype(jnp.float32)
    is_re = lax.rem(lax.broadcasted_iota(jnp.int32, (KMAX, rows), 1), 2 * KMAX) < KMAX
    line = weight_in[...]
    part_copies = []
    for slot in range(4):
        phi = arrived[slot].reshape(rows, quarter)
        psi = arrived[3 - slot].reshape(rows, quarter)
        wpsi = (psi.astype(jnp.float32) * line).astype(jnp.bfloat16)
        cross = times_transposed(wpsi, phi)
        cross = jnp.where(owner == partner_in[slot], cross, 0.0)
        chosen = jnp.sum(cross.reshape(freqs, 2 * KMAX, rows), axis=0)
        low, high = chosen[:KMAX], chosen[KMAX:]
        parts[slot] = jnp.where(
            is_re,
            low + pltpu.roll(high, rows - KMAX, 1),
            pltpu.roll(high, KMAX, 1) - low,
        )
        copy = remote(
            parts.at[slot],
            parts_in.at[slot],
            part_send.at[slot],
            part_recv.at[slot],
            meeting(slot)[0],
        )
        copy.start()
        part_copies.append(copy)
    for copy in part_copies:
        copy.wait_recv()
    sums[s] = (parts_in[0] + parts_in[1]) + (parts_in[2] + parts_in[3])
    for copy in sum_copies:
        copy.start()
    for copy in energy_copies:
        copy.wait_recv()
    energy_ref[...] = energies[...]
    for copy in sum_copies:
        copy.wait_recv()
    whole = sums[0]
    for place in range(1, n_space):
        whole = whole + sums[place]
    coherence_ref[...] = whole / total

    @pl.loop(0, n_chips)
    def _(step):
        core_copy(step).wait_send()

    @pl.loop(0, n_chips - 1)
    def _(step):
        chip_copy(step).wait_send()

    @pl.loop(0, freqs)
    def _(freq):
        for slot in range(4):
            mode_copy(freq, slot).wait_send()
        mode_store(freq).wait()

    sends = row_copies + coef_copies + energy_copies + part_copies + sum_copies
    for copy in [weight_copy] + sends:
        copy.wait_send()


def on_device(n_freq, n_space, spectra, weight, partner, counts):
    freqs, points, wide = spectra.shape
    half = wide // 2
    rows = 2 * KMAX
    lanes = rows * freqs
    quarter = points // 4
    n_chips = n_space // 2
    f32, bf16 = jnp.float32, jnp.bfloat16
    dma = pltpu.SemaphoreType.DMA
    vmem, smem = pltpu.VMEM, pltpu.SMEM
    modes, energy, coherence = pl.pallas_call(
        functools.partial(kernel, n_freq, n_space, points * n_space),
        out_shape=(
            jax.ShapeDtypeStruct((freqs, rows, points), bf16),
            jax.ShapeDtypeStruct((freqs, KMAX, 128), f32),
            jax.ShapeDtypeStruct((KMAX, lanes), f32),
        ),
        in_specs=[
            pl.BlockSpec(memory_space=pl.ANY),
            pl.BlockSpec(memory_space=vmem),
            pl.BlockSpec(memory_space=smem),
            pl.BlockSpec(memory_space=smem),
        ],
        out_specs=(
            pl.BlockSpec(memory_space=pl.ANY),
            pl.BlockSpec(memory_space=vmem),
            pl.BlockSpec(memory_space=vmem),
        ),
        scratch_shapes=[
            vmem((freqs, points, wide), bf16),
            vmem((points, 128), f32),
            vmem((points, wide), bf16),
            vmem((2 * n_chips, half, half), f32),
            vmem((n_chips, half, half), f32),
            vmem((n_chips, half, half), f32),
            vmem((rows, wide), bf16),
            vmem((freqs, rows, wide), bf16),
            vmem((KMAX, 128), f32),
            vmem((freqs, KMAX, 128), f32),
            vmem((freqs, rows, points), bf16),
            vmem((4, freqs, rows, quarter), bf16),
            vmem((4, 1, quarter), f32),
            vmem((1, quarter), f32),
            vmem((1, lanes), f32),
            vmem((4, 1, lanes), f32),
            vmem((4, KMAX, lanes), f32),
            vmem((4, KMAX, lanes), f32),
            vmem((n_space, KMAX, lanes), f32),
            dma((freqs,)),
            dma((freqs,)),
            dma((n_chips,)),
            dma((n_chips,)),
            dma((n_chips,)),
            dma((n_chips,)),
            dma((n_space,)),
            dma((n_space,)),
            dma((n_space,)),
            dma((n_space,)),
            dma((4, freqs)),
            dma((4, freqs)),
            dma((2,)),
            dma((4,)),
            dma((4,)),
            dma((4,)),
            dma((4,)),
            dma((n_space,)),
            dma((n_space,)),
        ],
        compiler_params=pltpu.CompilerParams(
            collective_id=0, has_side_effects=True, vmem_limit_bytes=60 * 1024 * 1024
        ),
    )(spectra, weight.reshape(points // 128, 128), partner, counts)
    coherence = coherence.reshape(KMAX, freqs, 2, KMAX).transpose(1, 2, 3, 0)
    return modes, energy[:, :, 0], coherence


def solution(mesh):
    in_specs = (P("freq", "space", None), P("space"), P("freq"), P("freq"))
    out_specs = (P("freq", None, "space"), P("freq", None), P("freq", None, None, None))
    body = functools.partial(on_device, mesh.shape["freq"], mesh.shape["space"])
    return jax.shard_map(
        body, mesh=mesh, in_specs=in_specs, out_specs=out_specs, check_vma=False
    )
```

```python
import functools

import jax
import jax.numpy as jnp
from jax import lax
from jax.experimental import pallas as pl
from jax.experimental.pallas import tpu as pltpu
from jax.sharding import PartitionSpec as P

KMAX = 8
ITERS = 4
EPS = 1e-06
AHEAD = 5
MESH = pl.DeviceIdType.MESH
HIGHEST = lax.Precision.HIGHEST


def moment(spectra, weight):
    turned = spectra.T.astype(jnp.float32) * weight
    return jnp.dot(turned.astype(jnp.bfloat16), spectra, preferred_element_type=jnp.float32)


def times_transposed(left, right):
    return lax.dot_general(
        left, right, (((1,), (1,)), ((), ())), preferred_element_type=jnp.float32
    )


def triangles(half):
    row = lax.broadcasted_iota(jnp.int32, (half, half), 0)
    col = lax.broadcasted_iota(jnp.int32, (half, half), 1)
    return row, col


def packed(moments):
    half = moments.shape[0] // 2
    row, col = triangles(half)
    gram_re = moments[:half, :half] + moments[half:, half:]
    gram_im = moments[:half, half:] - moments[half:, :half]
    return jnp.where(row <= col, gram_re, gram_im)


def unpacked(square, total):
    row, col = triangles(square.shape[0])
    flipped = square.T
    gram_re = jnp.where(row <= col, square, flipped)
    gram_im = jnp.where(row > col, square, jnp.where(row < col, -flipped, 0.0))
    return gram_re / total, gram_im / total


def orthonormal(vec_re, vec_im):
    ranks = lax.broadcasted_iota(jnp.int32, vec_re.shape, 0)
    for k in range(KMAX):
        own_re = jnp.broadcast_to(vec_re[k : k + 1], vec_re.shape)
        own_im = jnp.broadcast_to(vec_im[k : k + 1], vec_im.shape)
        norm = jnp.sum(own_re * own_re + own_im * own_im, axis=1, keepdims=True)
        proj_re = jnp.sum(own_re * vec_re + own_im * vec_im, axis=1, keepdims=True)
        proj_im = jnp.sum(own_re * vec_im - own_im * vec_re, axis=1, keepdims=True)
        inverse = lax.rsqrt(norm + EPS)
        unit_re, unit_im = own_re * inverse, own_im * inverse
        proj_re, proj_im = proj_re * inverse, proj_im * inverse
        new_re = vec_re - proj_re * unit_re + proj_im * unit_im
        new_im = vec_im - proj_re * unit_im - proj_im * unit_re
        vec_re = jnp.where(ranks > k, new_re, jnp.where(ranks == k, unit_re, vec_re))
        vec_im = jnp.where(ranks > k, new_im, jnp.where(ranks == k, unit_im, vec_im))
    return vec_re, vec_im


def solved(gram_re, gram_im, count):
    half = gram_re.shape[0]
    operator = jnp.concatenate([gram_re, gram_im], axis=1)

    def applied(vec_re, vec_im):
        both = jnp.concatenate([vec_re, vec_im], axis=0)
        image = jnp.dot(both, operator, precision=HIGHEST, preferred_element_type=jnp.float32)
        return (
            image[:KMAX, :half] + image[KMAX:, half:],
            image[KMAX:, :half] - image[:KMAX, half:],
        )

    vec_re, vec_im = orthonormal(gram_re[:KMAX], -gram_im[:KMAX])
    for _ in range(ITERS - 1):
        vec_re, vec_im = orthonormal(*applied(vec_re, vec_im))
    image_re, image_im = applied(vec_re, vec_im)
    energy = jnp.sum(vec_re * image_re + vec_im * image_im, axis=1, keepdims=True)
    ranks = lax.broadcasted_iota(jnp.int32, (KMAX, 1), 0)
    scale = jnp.where(ranks < count, lax.rsqrt(energy + EPS), 0.0)
    part_re, part_im = vec_re * scale, vec_im * scale
    coefficient = jnp.concatenate(
        [
            jnp.concatenate([part_re, -part_im], axis=1),
            jnp.concatenate([part_im, part_re], axis=1),
        ],
        axis=0,
    )
    return coefficient.astype(jnp.bfloat16), energy


def kernel(
    n_freq,
    n_space,
    total,
    spectra_hbm,
    weight_ref,
    partner_ref,
    counts_ref,
    modes_hbm,
    energy_ref,
    coherence_ref,
    spectra,
    squares,
    from_core,
    from_chips,
    coef_own,
    coefs,
    energy_own,
    energies,
    modes,
    arrived,
    weight_row,
    weight_in,
    partner_row,
    partner_in,
    parts,
    parts_in,
    sums,
    load_sem,
    store_sem,
    core_send,
    core_recv,
    chip_send,
    chip_recv,
    coef_send,
    coef_recv,
    energy_send,
    energy_recv,
    mode_send,
    mode_recv,
    weight_sem,
    row_send,
    row_recv,
    part_send,
    part_recv,
    sum_send,
    sum_recv,
):
    freqs, points, wide = spectra.shape
    quarter = points // 4
    g, s = lax.axis_index("freq"), lax.axis_index("space")
    core, chip = lax.rem(s, 2), s // 2
    n_chips = n_space // 2
    n_y = max(n_chips // 2, 1)
    z_lo, y = chip // n_y, lax.rem(chip, n_y)
    x, z_hi = g // 2, lax.rem(g, 2)
    n_x = n_freq // 2

    def remote(src, dst, send, recv, device):
        return pltpu.make_async_remote_copy(
            src_ref=src,
            dst_ref=dst,
            send_sem=send,
            recv_sem=recv,
            device_id=device,
            device_id_type=MESH,
        )

    def space_peer(offset):
        return (g, lax.rem(s + offset, n_space))

    other_s = lax.rem(s + n_space // 2, n_space)

    def meeting(slot):
        to_x = x if slot < 2 else n_x - 1 - x
        to_z = z_hi if slot % 2 == 0 else 1 - z_hi
        part = 2 * to_z + (2 * to_x) // n_x
        return (2 * to_x + to_z, other_s), part

    def chip_ahead(ahead):
        to_z = lax.rem(z_lo + ahead // n_y, 2)
        to_y = lax.rem(y + lax.rem(ahead, n_y), n_y)
        return to_z * n_y + to_y

    def chip_at(step):
        return chip_ahead(n_chips - 1 - step)

    def slot_at(step):
        pair, second = step // 2, lax.rem(step, 2) == 1
        early = jnp.where(pair == 0, 0, n_chips + pair - 1)
        late = jnp.where(pair == n_chips - 1, 2 * n_chips - 1, pair + 1)
        return jnp.where(second, late, early)

    def freq_at(step):
        slot = slot_at(step)
        first = slot < n_chips
        place = jnp.where(first, slot, slot - n_chips)
        return 2 * chip_at(place) + jnp.where(first, 1 - core, core)

    def load(step):
        freq = freq_at(step)
        return pltpu.make_async_copy(spectra_hbm.at[freq], spectra.at[freq], load_sem.at[freq])

    for step in range(min(AHEAD, freqs)):
        load(step).start()

    barrier = pltpu.get_barrier_semaphore()
    for offset in range(1, n_space):
        pl.semaphore_signal(barrier, inc=1, device_id=space_peer(offset), device_id_type=MESH)
    for slot in range(1, 4):
        pl.semaphore_signal(barrier, inc=1, device_id=meeting(slot)[0], device_id_type=MESH)

    for tile in range(points // 128):
        weight_row[:, tile * 128 : (tile + 1) * 128] = weight_ref[tile : tile + 1, :]
    lanes = partner_row.shape[1]
    which = lax.broadcasted_iota(jnp.int32, (1, lanes), 1) // (2 * KMAX)
    row = jnp.zeros((1, lanes), jnp.float32)
    for freq in range(freqs):
        row = jnp.where(which == freq, partner_ref[freq].astype(jnp.float32), row)
    partner_row[...] = row

    def core_copy(step):
        return remote(
            squares.at[step],
            from_core.at[step],
            core_send.at[step],
            core_recv.at[step],
            (g, s + 1 - 2 * core),
        )

    def chip_copy(step):
        return remote(
            squares.at[n_chips + step],
            from_chips.at[step],
            chip_send.at[step],
            chip_recv.at[step],
            (g, 2 * chip_at(step) + core),
        )

    def gram(*steps):
        for step in steps:
            load(step).wait()

            @pl.when(step + AHEAD < freqs)
            def _():
                load(step + AHEAD).start()

        for step in steps:
            squares[slot_at(step)] = packed(moment(spectra[freq_at(step)], weight_row[...]))

    def add_and_send(k):
        core_copy(k).wait_recv()
        squares[n_chips + k] = squares[n_chips + k] + from_core[k]
        chip_copy(k).start()

    gram(0, 1)
    pl.semaphore_wait(barrier, n_space - 1 + 3)
    core_copy(0).start()
    core_copy(1).start()

    @pl.loop(1, n_chips - 1)
    def _(pair):
        gram(2 * pair, 2 * pair + 1)
        core_copy(pair + 1).start()
        add_and_send(pair - 1)

    gram(2 * n_chips - 2)
    add_and_send(n_chips - 2)

    start = pl.multiple_of(meeting(0)[1] * quarter, 128)
    weight_copy = remote(
        weight_row.at[:, pl.ds(start, quarter)],
        weight_in,
        weight_sem.at[0],
        weight_sem.at[1],
        meeting(0)[0],
    )
    row_copies = [
        remote(
            partner_row, partner_in.at[slot], row_send.at[slot], row_recv.at[slot], meeting(slot)[0]
        )
        for slot in range(4)
    ]
    weight_copy.start()
    for copy in row_copies:
        copy.start()

    gram(2 * n_chips - 1)
    core_copy(n_chips - 1).wait_recv()
    square = squares[2 * n_chips - 1] + from_core[n_chips - 1]
    for step in range(n_chips - 1):
        chip_copy(step).wait_recv()
        square = square + from_chips[step]
    coefficient, energy = solved(*unpacked(square, total), counts_ref[s])
    coef_own[...] = coefficient
    coefs[s] = coefficient
    ranks = lax.broadcasted_iota(jnp.int32, (KMAX, 128), 0)
    lane = lax.broadcasted_iota(jnp.int32, (KMAX, 128), 1)
    energy = jnp.sum(jnp.where(ranks == lane, energy, 0.0), axis=0, keepdims=True)
    energy_own[...] = energy
    energies[s] = energy

    near = [ahead for ahead in (0, 1, 3, 4, 2, 5, 7, 6) if ahead < n_chips]
    peers = [2 * chip_ahead(ahead) + lax.rem(core + flip, 2) for ahead in near for flip in (0, 1)]
    peers = peers[1:]

    def coef_copy(peer, owner):
        send, recv = coef_send.at[peer], coef_recv.at[owner]
        return remote(coef_own, coefs.at[owner], send, recv, (g, peer))

    coef_copies, energy_copies, sum_copies = [], [], []
    for peer in peers:
        coef_copies.append(coef_copy(peer, s))
        send, recv = energy_send.at[peer], energy_recv.at[s]
        energy_copies.append(remote(energy_own, energies.at[s], send, recv, (g, peer)))
        send, recv = sum_send.at[peer], sum_recv.at[s]
        sum_copies.append(remote(sums.at[s], sums.at[s], send, recv, (g, peer)))
    for copy in coef_copies:
        copy.start()
    for copy in energy_copies:
        copy.start()

    def mode_copy(freq, slot):
        device, part = meeting(slot)
        start = pl.multiple_of(part * quarter, 128)
        return remote(
            modes.at[freq, :, pl.ds(start, quarter)],
            arrived.at[slot, freq],
            mode_send.at[slot, freq],
            mode_recv.at[slot, freq],
            device,
        )

    def mode_store(freq):
        return pltpu.make_async_copy(modes.at[freq], modes_hbm.at[freq], store_sem.at[freq])

    @pl.loop(0, freqs)
    def _(step):
        ahead = jnp.int32(near[0])
        for place in range(1, n_chips):
            ahead = jnp.where(step // 2 == place, near[place], ahead)
        freq = 2 * chip_ahead(ahead) + lax.rem(core + step, 2)

        @pl.when(step > 0)
        def _():
            coef_copy(freq, freq).wait_recv()

        modes[freq] = times_transposed(coefs[freq], spectra[freq]).astype(jnp.bfloat16)
        for slot in (2, 3, 0, 1):
            mode_copy(freq, slot).start()
        mode_store(freq).start()

    for copy in row_copies:
        copy.wait_recv()
    weight_copy.wait_recv()

    @pl.loop(0, freqs)
    def _(freq):
        for slot in range(4):
            mode_copy(freq, slot).wait_recv()

    rows = 2 * KMAX * freqs
    owner = lax.broadcasted_iota(jnp.int32, (rows, rows), 0) // (2 * KMAX)
    owner = owner.astype(jnp.float32)
    is_re = lax.rem(lax.broadcasted_iota(jnp.int32, (KMAX, rows), 1), 2 * KMAX) < KMAX
    line = weight_in[...]
    part_copies = []
    for slot in range(4):
        phi = arrived[slot].reshape(rows, quarter)
        psi = arrived[3 - slot].reshape(rows, quarter)
        wpsi = (psi.astype(jnp.float32) * line).astype(jnp.bfloat16)
        cross = times_transposed(wpsi, phi)
        cross = jnp.where(owner == partner_in[slot], cross, 0.0)
        chosen = jnp.sum(cross.reshape(freqs, 2 * KMAX, rows), axis=0)
        low, high = chosen[:KMAX], chosen[KMAX:]
        parts[slot] = jnp.where(
            is_re,
            low + pltpu.roll(high, rows - KMAX, 1),
            pltpu.roll(high, KMAX, 1) - low,
        )
        copy = remote(
            parts.at[slot],
            parts_in.at[slot],
            part_send.at[slot],
            part_recv.at[slot],
            meeting(slot)[0],
        )
        copy.start()
        part_copies.append(copy)
    for copy in part_copies:
        copy.wait_recv()
    sums[s] = (parts_in[0] + parts_in[1]) + (parts_in[2] + parts_in[3])
    for copy in sum_copies:
        copy.start()
    for peer in peers:
        send, recv = energy_send.at[peer], energy_recv.at[peer]
        remote(energy_own, energies.at[peer], send, recv, (g, peer)).wait_recv()
    gathered = jnp.concatenate([energies[k] for k in range(freqs)], axis=0)
    energy_ref[...] = gathered.T[:KMAX]

    old = lax.broadcasted_iota(jnp.int32, (lanes, lanes), 0)
    new = lax.broadcasted_iota(jnp.int32, (lanes, lanes), 1)
    both = 2 * KMAX
    moves = jnp.logical_and(old // both == lax.rem(new, freqs), lax.rem(old, both) == new // freqs)
    moves = jnp.where(moves, 1.0, 0.0).astype(jnp.bfloat16)
    for peer in peers:
        send, recv = sum_send.at[peer], sum_recv.at[peer]
        remote(sums.at[s], sums.at[peer], send, recv, (g, peer)).wait_recv()
    whole = sums[0]
    for place in range(1, n_space):
        whole = whole + sums[place]
    whole = whole / total
    high = whole.astype(jnp.bfloat16).astype(jnp.float32)
    mid = (whole - high).astype(jnp.bfloat16).astype(jnp.float32)
    pieces = jnp.concatenate([high, mid, whole - high - mid, jnp.zeros_like(whole)], axis=0)
    moved = jnp.dot(pieces.astype(jnp.bfloat16), moves, preferred_element_type=jnp.float32)
    moved = moved[:KMAX] + (moved[KMAX : 2 * KMAX] + moved[2 * KMAX : 3 * KMAX])
    for place in range(both):
        piece = moved[:, place * freqs : (place + 1) * freqs]
        coherence_ref[place // KMAX, place % KMAX] = piece

    @pl.loop(0, n_chips)
    def _(step):
        core_copy(step).wait_send()

    @pl.loop(0, n_chips - 1)
    def _(step):
        chip_copy(step).wait_send()

    @pl.loop(0, freqs)
    def _(freq):
        for slot in range(4):
            mode_copy(freq, slot).wait_send()
        mode_store(freq).wait()

    sends = row_copies + coef_copies + energy_copies + part_copies + sum_copies
    for copy in [weight_copy] + sends:
        copy.wait_send()


def hand_on(modes_in, energy_in, coherence_in, modes_out, energy_out, coherence_out, held, ins, outs):
    freqs = held.shape[0]

    def taken(freq):
        return pltpu.make_async_copy(modes_in.at[freq], held.at[freq], ins.at[freq])

    def given(freq):
        return pltpu.make_async_copy(held.at[freq], modes_out.at[freq], outs.at[freq])

    for freq in range(freqs):
        taken(freq).start()
    energy_out[...] = energy_in[...]
    coherence_out[...] = coherence_in[...]
    for freq in range(freqs):
        taken(freq).wait()
        given(freq).start()
    for freq in range(freqs):
        given(freq).wait()


def on_device(n_freq, n_space, spectra, weight, partner, counts):
    freqs, points, wide = spectra.shape
    half = wide // 2
    rows = 2 * KMAX
    lanes = rows * freqs
    quarter = points // 4
    n_chips = n_space // 2
    f32, bf16 = jnp.float32, jnp.bfloat16
    dma = pltpu.SemaphoreType.DMA
    vmem, smem = pltpu.VMEM, pltpu.SMEM
    modes, energy, coherence = pl.pallas_call(
        functools.partial(kernel, n_freq, n_space, points * n_space),
        out_shape=(
            jax.ShapeDtypeStruct((freqs, rows, points), bf16),
            jax.ShapeDtypeStruct((KMAX, freqs), f32),
            jax.ShapeDtypeStruct((2, KMAX, KMAX, freqs), f32),
        ),
        in_specs=[
            pl.BlockSpec(memory_space=pl.ANY),
            pl.BlockSpec(memory_space=vmem),
            pl.BlockSpec(memory_space=smem),
            pl.BlockSpec(memory_space=smem),
        ],
        out_specs=(
            pl.BlockSpec(memory_space=pltpu.HBM),
            pl.BlockSpec(memory_space=vmem),
            pl.BlockSpec(memory_space=vmem),
        ),
        scratch_shapes=[
            vmem((freqs, points, wide), bf16),
            vmem((2 * n_chips, half, half), f32),
            vmem((n_chips, half, half), f32),
            vmem((n_chips, half, half), f32),
            vmem((rows, wide), bf16),
            vmem((freqs, rows, wide), bf16),
            vmem((1, 128), f32),
            vmem((freqs, 1, 128), f32),
            vmem((freqs, rows, points), bf16),
            vmem((4, freqs, rows, quarter), bf16),
            vmem((1, points), f32),
            vmem((1, quarter), f32),
            vmem((1, lanes), f32),
            vmem((4, 1, lanes), f32),
            vmem((4, KMAX, lanes), f32),
            vmem((4, KMAX, lanes), f32),
            vmem((n_space, KMAX, lanes), f32),
            dma((freqs,)),
            dma((freqs,)),
            dma((n_chips,)),
            dma((n_chips,)),
            dma((n_chips,)),
            dma((n_chips,)),
            dma((n_space,)),
            dma((n_space,)),
            dma((n_space,)),
            dma((n_space,)),
            dma((4, freqs)),
            dma((4, freqs)),
            dma((2,)),
            dma((4,)),
            dma((4,)),
            dma((4,)),
            dma((4,)),
            dma((n_space,)),
            dma((n_space,)),
        ],
        compiler_params=pltpu.CompilerParams(
            collective_id=0, has_side_effects=True, vmem_limit_bytes=60 * 1024 * 1024
        ),
    )(spectra, weight.reshape(points // 128, 128), partner, counts)
    outs = (modes, energy, coherence)
    modes, energy, coherence = pl.pallas_call(
        hand_on,
        out_shape=tuple(jax.ShapeDtypeStruct(out.shape, out.dtype) for out in outs),
        in_specs=[
            pl.BlockSpec(memory_space=pltpu.HBM),
            pl.BlockSpec(memory_space=vmem),
            pl.BlockSpec(memory_space=vmem),
        ],
        out_specs=(
            pl.BlockSpec(memory_space=pltpu.HBM),
            pl.BlockSpec(memory_space=vmem),
            pl.BlockSpec(memory_space=vmem),
        ),
        scratch_shapes=[vmem(modes.shape, bf16), dma((freqs,)), dma((freqs,))],
    )(*outs)
    return modes, energy.T, coherence.transpose(3, 0, 1, 2)


def solution(mesh):
    in_specs = (P("freq", "space", None), P("space"), P("freq"), P("freq"))
    out_specs = (P("freq", None, "space"), P("freq", None), P("freq", None, None, None))
    body = functools.partial(on_device, mesh.shape["freq"], mesh.shape["space"])
    return jax.shard_map(
        body, mesh=mesh, in_specs=in_specs, out_specs=out_specs, check_vma=False
    )
```

```python
import functools

import jax
import jax.numpy as jnp
from jax import lax
from jax.experimental import pallas as pl
from jax.experimental.pallas import tpu as pltpu
from jax.sharding import PartitionSpec as P

KMAX = 8
ITERS = 4
EPS = 1e-06
AHEAD = 5
MESH = pl.DeviceIdType.MESH
HIGHEST = lax.Precision.HIGHEST


def moment(spectra, weight):
    turned = spectra.T.astype(jnp.float32) * weight
    return jnp.dot(turned.astype(jnp.bfloat16), spectra, preferred_element_type=jnp.float32)


def times_transposed(left, right):
    return lax.dot_general(
        left, right, (((1,), (1,)), ((), ())), preferred_element_type=jnp.float32
    )


def triangles(half):
    row = lax.broadcasted_iota(jnp.int32, (half, half), 0)
    col = lax.broadcasted_iota(jnp.int32, (half, half), 1)
    return row, col


def packed(moments):
    half = moments.shape[0] // 2
    row, col = triangles(half)
    gram_re = moments[:half, :half] + moments[half:, half:]
    gram_im = moments[:half, half:] - moments[half:, :half]
    return jnp.where(row <= col, gram_re, gram_im)


def unpacked(square, total):
    row, col = triangles(square.shape[0])
    flipped = square.T
    gram_re = jnp.where(row <= col, square, flipped)
    gram_im = jnp.where(row > col, square, jnp.where(row < col, -flipped, 0.0))
    return gram_re / total, gram_im / total


def orthonormal(vec_re, vec_im):
    ranks = lax.broadcasted_iota(jnp.int32, vec_re.shape, 0)
    for k in range(KMAX):
        own_re = jnp.broadcast_to(vec_re[k : k + 1], vec_re.shape)
        own_im = jnp.broadcast_to(vec_im[k : k + 1], vec_im.shape)
        norm = jnp.sum(own_re * own_re + own_im * own_im, axis=1, keepdims=True)
        proj_re = jnp.sum(own_re * vec_re + own_im * vec_im, axis=1, keepdims=True)
        proj_im = jnp.sum(own_re * vec_im - own_im * vec_re, axis=1, keepdims=True)
        inverse = lax.rsqrt(norm + EPS)
        unit_re, unit_im = own_re * inverse, own_im * inverse
        proj_re, proj_im = proj_re * inverse, proj_im * inverse
        new_re = vec_re - proj_re * unit_re + proj_im * unit_im
        new_im = vec_im - proj_re * unit_im - proj_im * unit_re
        vec_re = jnp.where(ranks > k, new_re, jnp.where(ranks == k, unit_re, vec_re))
        vec_im = jnp.where(ranks > k, new_im, jnp.where(ranks == k, unit_im, vec_im))
    return vec_re, vec_im


def solved(gram_re, gram_im, count):
    half = gram_re.shape[0]
    operator = jnp.concatenate([gram_re, gram_im], axis=1)

    def applied(vec_re, vec_im):
        both = jnp.concatenate([vec_re, vec_im], axis=0)
        image = jnp.dot(both, operator, precision=HIGHEST, preferred_element_type=jnp.float32)
        return (
            image[:KMAX, :half] + image[KMAX:, half:],
            image[KMAX:, :half] - image[:KMAX, half:],
        )

    vec_re, vec_im = orthonormal(gram_re[:KMAX], -gram_im[:KMAX])
    for _ in range(ITERS - 1):
        vec_re, vec_im = orthonormal(*applied(vec_re, vec_im))
    image_re, image_im = applied(vec_re, vec_im)
    energy = jnp.sum(vec_re * image_re + vec_im * image_im, axis=1, keepdims=True)
    ranks = lax.broadcasted_iota(jnp.int32, (KMAX, 1), 0)
    scale = jnp.where(ranks < count, lax.rsqrt(energy + EPS), 0.0)
    part_re, part_im = vec_re * scale, vec_im * scale
    coefficient = jnp.concatenate(
        [
            jnp.concatenate([part_re, -part_im], axis=1),
            jnp.concatenate([part_im, part_re], axis=1),
        ],
        axis=0,
    )
    return coefficient.astype(jnp.bfloat16), energy


def kernel(
    n_freq,
    n_space,
    total,
    spectra_hbm,
    weight_ref,
    partner_ref,
    counts_ref,
    modes_hbm,
    energy_ref,
    coherence_ref,
    spectra,
    squares,
    from_core,
    from_chips,
    coef_own,
    coefs,
    energy_own,
    energies,
    modes,
    arrived,
    weight_row,
    weight_in,
    partner_row,
    partner_in,
    parts,
    parts_in,
    sums,
    load_sem,
    store_sem,
    core_send,
    core_recv,
    chip_send,
    chip_recv,
    coef_send,
    coef_recv,
    energy_send,
    energy_recv,
    mode_send,
    mode_recv,
    weight_sem,
    row_send,
    row_recv,
    part_send,
    part_recv,
    sum_send,
    sum_recv,
):
    freqs, points, wide = spectra.shape
    quarter = points // 4
    g, s = lax.axis_index("freq"), lax.axis_index("space")
    core, chip = lax.rem(s, 2), s // 2
    n_chips = n_space // 2
    n_y = max(n_chips // 2, 1)
    z_lo, y = chip // n_y, lax.rem(chip, n_y)
    x, z_hi = g // 2, lax.rem(g, 2)
    n_x = n_freq // 2

    def remote(src, dst, send, recv, device):
        return pltpu.make_async_remote_copy(
            src_ref=src,
            dst_ref=dst,
            send_sem=send,
            recv_sem=recv,
            device_id=device,
            device_id_type=MESH,
        )

    def space_peer(offset):
        return (g, lax.rem(s + offset, n_space))

    other_s = lax.rem(s + n_space // 2, n_space)

    def meeting(slot):
        to_x = x if slot < 2 else n_x - 1 - x
        to_z = z_hi if slot % 2 == 0 else 1 - z_hi
        part = 2 * to_z + (2 * to_x) // n_x
        return (2 * to_x + to_z, other_s), part

    def chip_ahead(ahead):
        to_z = lax.rem(z_lo + ahead // n_y, 2)
        to_y = lax.rem(y + lax.rem(ahead, n_y), n_y)
        return to_z * n_y + to_y

    def chip_at(k):
        return chip_ahead(n_chips - 1 - k)

    def place_at(step):
        step = jnp.int32(step)
        last = step == 2 * n_chips - 1
        early = step < n_chips - 1
        own_even = jnp.logical_or(early, last)
        k_even = jnp.where(early, step, jnp.where(last, n_chips - 1, step - (n_chips - 1)))
        own = jnp.where(core == 0, own_even.astype(jnp.int32), (step >= n_chips).astype(jnp.int32))
        return own, jnp.where(core == 0, k_even, lax.rem(step, n_chips))

    def slot_at(step):
        own, k = place_at(step)
        return own * n_chips + k

    def freq_at(step):
        own, k = place_at(step)
        return 2 * chip_at(k) + jnp.where(own == 1, core, 1 - core)

    def load(step):
        freq = freq_at(step)
        return pltpu.make_async_copy(spectra_hbm.at[freq], spectra.at[freq], load_sem.at[freq])

    for step in range(min(AHEAD, freqs)):
        load(step).start()

    barrier = pltpu.get_barrier_semaphore()
    for offset in range(1, n_space):
        pl.semaphore_signal(barrier, inc=1, device_id=space_peer(offset), device_id_type=MESH)
    for slot in range(1, 4):
        pl.semaphore_signal(barrier, inc=1, device_id=meeting(slot)[0], device_id_type=MESH)

    for tile in range(points // 128):
        weight_row[:, tile * 128 : (tile + 1) * 128] = weight_ref[tile : tile + 1, :]
    lanes = partner_row.shape[1]
    which = lax.broadcasted_iota(jnp.int32, (1, lanes), 1) // (2 * KMAX)
    row = jnp.zeros((1, lanes), jnp.float32)
    for freq in range(freqs):
        row = jnp.where(which == freq, partner_ref[freq].astype(jnp.float32), row)
    partner_row[...] = row

    def core_copy(step):
        return remote(
            squares.at[step],
            from_core.at[step],
            core_send.at[step],
            core_recv.at[step],
            (g, s + 1 - 2 * core),
        )

    def chip_copy(step):
        return remote(
            squares.at[n_chips + step],
            from_chips.at[step],
            chip_send.at[step],
            chip_recv.at[step],
            (g, 2 * chip_at(step) + core),
        )

    def gram(*steps):
        for step in steps:
            load(step).wait()

            @pl.when(step + AHEAD < freqs)
            def _():
                load(step + AHEAD).start()

        for step in steps:
            squares[slot_at(step)] = packed(moment(spectra[freq_at(step)], weight_row[...]))

    def hand_over(step):
        own, k = place_at(step)

        @pl.when(own == 0)
        def _():
            core_copy(k).start()

    def add_and_send(step):
        own, k = place_at(step)

        @pl.when(own == 1)
        def _():
            core_copy(k).wait_recv()
            squares[n_chips + k] = squares[n_chips + k] + from_core[k]
            chip_copy(k).start()

    gram(0, 1)
    pl.semaphore_wait(barrier, n_space - 1 + 3)
    hand_over(0)
    hand_over(1)

    @pl.loop(1, n_chips - 1)
    def _(pair):
        gram(2 * pair, 2 * pair + 1)
        hand_over(2 * pair)
        hand_over(2 * pair + 1)
        add_and_send(2 * pair - 2 + core)
        add_and_send(2 * pair - 1 + core)

    gram(2 * n_chips - 2)
    hand_over(2 * n_chips - 2)
    add_and_send(2 * n_chips - 4 + core)
    add_and_send(2 * n_chips - 3 + core)

    start = pl.multiple_of(meeting(0)[1] * quarter, 128)
    weight_copy = remote(
        weight_row.at[:, pl.ds(start, quarter)],
        weight_in,
        weight_sem.at[0],
        weight_sem.at[1],
        meeting(0)[0],
    )
    row_copies = [
        remote(
            partner_row, partner_in.at[slot], row_send.at[slot], row_recv.at[slot], meeting(slot)[0]
        )
        for slot in range(4)
    ]
    weight_copy.start()
    for copy in row_copies:
        copy.start()

    gram(2 * n_chips - 1)
    core_copy(n_chips - 1).wait_recv()
    square = squares[2 * n_chips - 1] + from_core[n_chips - 1]
    for step in range(n_chips - 1):
        chip_copy(step).wait_recv()
        square = square + from_chips[step]
    coefficient, energy = solved(*unpacked(square, total), counts_ref[s])
    coef_own[...] = coefficient
    coefs[s] = coefficient
    ranks = lax.broadcasted_iota(jnp.int32, (KMAX, 128), 0)
    lane = lax.broadcasted_iota(jnp.int32, (KMAX, 128), 1)
    energy = jnp.sum(jnp.where(ranks == lane, energy, 0.0), axis=0, keepdims=True)
    energy_own[...] = energy
    energies[s] = energy

    near = [ahead for ahead in (0, 1, 3, 4, 2, 5, 7, 6) if ahead < n_chips]
    peers = [2 * chip_ahead(ahead) + lax.rem(core + flip, 2) for ahead in near for flip in (0, 1)]
    peers = peers[1:]

    def coef_copy(peer, owner):
        send, recv = coef_send.at[peer], coef_recv.at[owner]
        return remote(coef_own, coefs.at[owner], send, recv, (g, peer))

    coef_copies, energy_copies, sum_copies = [], [], []
    for peer in peers:
        coef_copies.append(coef_copy(peer, s))
        send, recv = energy_send.at[peer], energy_recv.at[s]
        energy_copies.append(remote(energy_own, energies.at[s], send, recv, (g, peer)))
        send, recv = sum_send.at[peer], sum_recv.at[s]
        sum_copies.append(remote(sums.at[s], sums.at[s], send, recv, (g, peer)))
    for copy in coef_copies:
        copy.start()
    for copy in energy_copies:
        copy.start()

    def mode_copy(freq, slot):
        device, part = meeting(slot)
        start = pl.multiple_of(part * quarter, 128)
        return remote(
            modes.at[freq, :, pl.ds(start, quarter)],
            arrived.at[slot, freq],
            mode_send.at[slot, freq],
            mode_recv.at[slot, freq],
            device,
        )

    def mode_store(freq):
        return pltpu.make_async_copy(modes.at[freq], modes_hbm.at[freq], store_sem.at[freq])

    @pl.loop(0, freqs)
    def _(step):
        even = step < n_chips + core
        place = jnp.where(step == 0, 0, jnp.where(even, step - core, step - n_chips))
        parity = jnp.where(step == 0, core, jnp.where(even, 0, 1))
        ahead = jnp.int32(near[0])
        for spot in range(1, n_chips):
            ahead = jnp.where(place == spot, near[spot], ahead)
        freq = 2 * chip_ahead(ahead) + parity

        @pl.when(step > 0)
        def _():
            coef_copy(freq, freq).wait_recv()

        modes[freq] = times_transposed(coefs[freq], spectra[freq]).astype(jnp.bfloat16)
        for slot in (2, 3, 0, 1):
            mode_copy(freq, slot).start()
        mode_store(freq).start()

    for copy in row_copies:
        copy.wait_recv()
    weight_copy.wait_recv()

    @pl.loop(0, freqs)
    def _(freq):
        for slot in range(4):
            mode_copy(freq, slot).wait_recv()

    rows = 2 * KMAX * freqs
    owner = lax.broadcasted_iota(jnp.int32, (rows, rows), 0) // (2 * KMAX)
    owner = owner.astype(jnp.float32)
    is_re = lax.rem(lax.broadcasted_iota(jnp.int32, (KMAX, rows), 1), 2 * KMAX) < KMAX
    line = weight_in[...]
    part_copies = []
    for slot in range(4):
        phi = arrived[slot].reshape(rows, quarter)
        psi = arrived[3 - slot].reshape(rows, quarter)
        wpsi = (psi.astype(jnp.float32) * line).astype(jnp.bfloat16)
        cross = times_transposed(wpsi, phi)
        cross = jnp.where(owner == partner_in[slot], cross, 0.0)
        chosen = jnp.sum(cross.reshape(freqs, 2 * KMAX, rows), axis=0)
        low, high = chosen[:KMAX], chosen[KMAX:]
        parts[slot] = jnp.where(
            is_re,
            low + pltpu.roll(high, rows - KMAX, 1),
            pltpu.roll(high, KMAX, 1) - low,
        )
        copy = remote(
            parts.at[slot],
            parts_in.at[slot],
            part_send.at[slot],
            part_recv.at[slot],
            meeting(slot)[0],
        )
        copy.start()
        part_copies.append(copy)
    for copy in part_copies:
        copy.wait_recv()
    sums[s] = (parts_in[0] + parts_in[1]) + (parts_in[2] + parts_in[3])
    for copy in sum_copies:
        copy.start()
    for peer in peers:
        send, recv = energy_send.at[peer], energy_recv.at[peer]
        remote(energy_own, energies.at[peer], send, recv, (g, peer)).wait_recv()
    gathered = jnp.concatenate([energies[k] for k in range(freqs)], axis=0)
    energy_ref[...] = gathered.T[:KMAX]

    old = lax.broadcasted_iota(jnp.int32, (lanes, lanes), 0)
    new = lax.broadcasted_iota(jnp.int32, (lanes, lanes), 1)
    both = 2 * KMAX
    moves = jnp.logical_and(old // both == lax.rem(new, freqs), lax.rem(old, both) == new // freqs)
    moves = jnp.where(moves, 1.0, 0.0).astype(jnp.bfloat16)
    for peer in peers:
        send, recv = sum_send.at[peer], sum_recv.at[peer]
        remote(sums.at[s], sums.at[peer], send, recv, (g, peer)).wait_recv()
    whole = sums[0]
    for place in range(1, n_space):
        whole = whole + sums[place]
    whole = whole / total
    high = whole.astype(jnp.bfloat16).astype(jnp.float32)
    mid = (whole - high).astype(jnp.bfloat16).astype(jnp.float32)
    pieces = jnp.concatenate([high, mid, whole - high - mid, jnp.zeros_like(whole)], axis=0)
    moved = jnp.dot(pieces.astype(jnp.bfloat16), moves, preferred_element_type=jnp.float32)
    moved = moved[:KMAX] + (moved[KMAX : 2 * KMAX] + moved[2 * KMAX : 3 * KMAX])
    for place in range(both):
        piece = moved[:, place * freqs : (place + 1) * freqs]
        coherence_ref[place // KMAX, place % KMAX] = piece

    @pl.loop(0, n_chips)
    def _(step):
        core_copy(step).wait_send()

    @pl.loop(0, n_chips - 1)
    def _(step):
        chip_copy(step).wait_send()

    @pl.loop(0, freqs)
    def _(freq):
        for slot in range(4):
            mode_copy(freq, slot).wait_send()
        mode_store(freq).wait()

    sends = row_copies + coef_copies + energy_copies + part_copies + sum_copies
    for copy in [weight_copy] + sends:
        copy.wait_send()


def hand_on(*refs):
    sources, targets, held = refs[:3], refs[3:6], refs[6:9]
    small, modes = (1, 2), range(held[0].shape[0])
    ins, outs = refs[9:]

    def copies(start, end, sems):
        rows = [pltpu.make_async_copy(start[k], end[k], sems.at[k]) for k in small]
        for freq in modes:
            rows.append(pltpu.make_async_copy(start[0].at[freq], end[0].at[freq], sems.at[3 + freq]))
        return rows

    taken, given = copies(sources, held, ins), copies(held, targets, outs)
    for copy in taken:
        copy.start()
    for first, second in zip(taken, given):
        first.wait()
        second.start()
    for copy in given:
        copy.wait()


def on_device(n_freq, n_space, spectra, weight, partner, counts):
    freqs, points, wide = spectra.shape
    half = wide // 2
    rows = 2 * KMAX
    lanes = rows * freqs
    quarter = points // 4
    n_chips = n_space // 2
    f32, bf16 = jnp.float32, jnp.bfloat16
    dma = pltpu.SemaphoreType.DMA
    vmem, smem = pltpu.VMEM, pltpu.SMEM
    modes, energy, coherence = pl.pallas_call(
        functools.partial(kernel, n_freq, n_space, points * n_space),
        out_shape=(
            jax.ShapeDtypeStruct((freqs, rows, points), bf16),
            jax.ShapeDtypeStruct((KMAX, freqs), f32),
            jax.ShapeDtypeStruct((2, KMAX, KMAX, freqs), f32),
        ),
        in_specs=[
            pl.BlockSpec(memory_space=pl.ANY),
            pl.BlockSpec(memory_space=vmem),
            pl.BlockSpec(memory_space=smem),
            pl.BlockSpec(memory_space=smem),
        ],
        out_specs=(
            pl.BlockSpec(memory_space=pltpu.HBM),
            pl.BlockSpec(memory_space=vmem),
            pl.BlockSpec(memory_space=vmem),
        ),
        scratch_shapes=[
            vmem((freqs, points, wide), bf16),
            vmem((2 * n_chips, half, half), f32),
            vmem((n_chips, half, half), f32),
            vmem((n_chips, half, half), f32),
            vmem((rows, wide), bf16),
            vmem((freqs, rows, wide), bf16),
            vmem((1, 128), f32),
            vmem((freqs, 1, 128), f32),
            vmem((freqs, rows, points), bf16),
            vmem((4, freqs, rows, quarter), bf16),
            vmem((1, points), f32),
            vmem((1, quarter), f32),
            vmem((1, lanes), f32),
            vmem((4, 1, lanes), f32),
            vmem((4, KMAX, lanes), f32),
            vmem((4, KMAX, lanes), f32),
            vmem((n_space, KMAX, lanes), f32),
            dma((freqs,)),
            dma((freqs,)),
            dma((n_chips,)),
            dma((n_chips,)),
            dma((n_chips,)),
            dma((n_chips,)),
            dma((n_space,)),
            dma((n_space,)),
            dma((n_space,)),
            dma((n_space,)),
            dma((4, freqs)),
            dma((4, freqs)),
            dma((2,)),
            dma((4,)),
            dma((4,)),
            dma((4,)),
            dma((4,)),
            dma((n_space,)),
            dma((n_space,)),
        ],
        compiler_params=pltpu.CompilerParams(
            collective_id=0, has_side_effects=True, vmem_limit_bytes=60 * 1024 * 1024
        ),
    )(spectra, weight.reshape(points // 128, 128), partner, counts)
    outs = (modes, energy, coherence)
    modes, energy, coherence = pl.pallas_call(
        hand_on,
        out_shape=tuple(jax.ShapeDtypeStruct(out.shape, out.dtype) for out in outs),
        in_specs=[pl.BlockSpec(memory_space=pltpu.HBM)] * 3,
        out_specs=(pl.BlockSpec(memory_space=pltpu.HBM),) * 3,
        scratch_shapes=[vmem(out.shape, out.dtype) for out in outs]
        + [dma((3 + freqs,)), dma((3 + freqs,))],
    )(*outs)
    return modes, energy.T, coherence.transpose(3, 0, 1, 2)


def solution(mesh):
    in_specs = (P("freq", "space", None), P("space"), P("freq"), P("freq"))
    out_specs = (P("freq", None, "space"), P("freq", None), P("freq", None, None, None))
    body = functools.partial(on_device, mesh.shape["freq"], mesh.shape["space"])
    return jax.shard_map(
        body, mesh=mesh, in_specs=in_specs, out_specs=out_specs, check_vma=False
    )
```

```python
import functools

import jax
import jax.numpy as jnp
from jax import lax
from jax.experimental import pallas as pl
from jax.experimental.pallas import tpu as pltpu
from jax.sharding import PartitionSpec as P

KMAX = 8
ITERS = 4
EPS = 1e-06
AHEAD = 5
EARLY = 1
MESH = pl.DeviceIdType.MESH
HIGHEST = lax.Precision.HIGHEST


def moment(spectra, weight):
    turned = spectra.T.astype(jnp.float32) * weight
    return jnp.dot(turned.astype(jnp.bfloat16), spectra, preferred_element_type=jnp.float32)


def times_transposed(left, right):
    return lax.dot_general(
        left, right, (((1,), (1,)), ((), ())), preferred_element_type=jnp.float32
    )


def triangles(half):
    row = lax.broadcasted_iota(jnp.int32, (half, half), 0)
    col = lax.broadcasted_iota(jnp.int32, (half, half), 1)
    return row, col


def packed(moments):
    half = moments.shape[0] // 2
    row, col = triangles(half)
    gram_re = moments[:half, :half] + moments[half:, half:]
    gram_im = moments[:half, half:] - moments[half:, :half]
    return jnp.where(row <= col, gram_re, gram_im)


def unpacked(square, total):
    row, col = triangles(square.shape[0])
    flipped = square.T
    gram_re = jnp.where(row <= col, square, flipped)
    gram_im = jnp.where(row > col, square, jnp.where(row < col, -flipped, 0.0))
    return gram_re / total, gram_im / total


def orthonormal(vec_re, vec_im):
    ranks = lax.broadcasted_iota(jnp.int32, vec_re.shape, 0)
    for k in range(KMAX):
        own_re = jnp.broadcast_to(vec_re[k : k + 1], vec_re.shape)
        own_im = jnp.broadcast_to(vec_im[k : k + 1], vec_im.shape)
        norm = jnp.sum(own_re * own_re + own_im * own_im, axis=1, keepdims=True)
        proj_re = jnp.sum(own_re * vec_re + own_im * vec_im, axis=1, keepdims=True)
        proj_im = jnp.sum(own_re * vec_im - own_im * vec_re, axis=1, keepdims=True)
        inverse = lax.rsqrt(norm + EPS)
        unit_re, unit_im = own_re * inverse, own_im * inverse
        proj_re, proj_im = proj_re * inverse, proj_im * inverse
        new_re = vec_re - proj_re * unit_re + proj_im * unit_im
        new_im = vec_im - proj_re * unit_im - proj_im * unit_re
        vec_re = jnp.where(ranks > k, new_re, jnp.where(ranks == k, unit_re, vec_re))
        vec_im = jnp.where(ranks > k, new_im, jnp.where(ranks == k, unit_im, vec_im))
    return vec_re, vec_im


def solved(gram_re, gram_im, count):
    half = gram_re.shape[0]
    operator = jnp.concatenate([gram_re, gram_im], axis=1)

    def applied(vec_re, vec_im):
        both = jnp.concatenate([vec_re, vec_im], axis=0)
        image = jnp.dot(both, operator, precision=HIGHEST, preferred_element_type=jnp.float32)
        return (
            image[:KMAX, :half] + image[KMAX:, half:],
            image[KMAX:, :half] - image[:KMAX, half:],
        )

    vec_re, vec_im = orthonormal(gram_re[:KMAX], -gram_im[:KMAX])
    for _ in range(ITERS - 1):
        vec_re, vec_im = orthonormal(*applied(vec_re, vec_im))
    image_re, image_im = applied(vec_re, vec_im)
    energy = jnp.sum(vec_re * image_re + vec_im * image_im, axis=1, keepdims=True)
    ranks = lax.broadcasted_iota(jnp.int32, (KMAX, 1), 0)
    scale = jnp.where(ranks < count, lax.rsqrt(energy + EPS), 0.0)
    part_re, part_im = vec_re * scale, vec_im * scale
    return jnp.concatenate([part_re, -part_im], axis=1).astype(jnp.bfloat16), energy


def both_halves(upper):
    half = upper.shape[1] // 2
    upper = upper.astype(jnp.float32)
    lower = jnp.concatenate([-upper[:, half:], upper[:, :half]], axis=1)
    return jnp.concatenate([upper, lower], axis=0).astype(jnp.bfloat16)


def kernel(
    n_freq,
    n_space,
    total,
    spectra_hbm,
    weight_ref,
    partner_ref,
    counts_ref,
    modes_hbm,
    energy_ref,
    coherence_ref,
    spectra,
    squares,
    from_core,
    from_chips,
    coef_own,
    coefs,
    energy_own,
    energies,
    modes,
    arrived,
    weight_row,
    weight_in,
    partner_row,
    partner_in,
    parts,
    parts_in,
    sums,
    load_sem,
    store_sem,
    core_send,
    core_recv,
    chip_send,
    chip_recv,
    coef_send,
    coef_recv,
    energy_send,
    energy_recv,
    mode_send,
    mode_recv,
    weight_sem,
    row_send,
    row_recv,
    part_send,
    part_recv,
    sum_send,
    sum_recv,
):
    freqs, points, wide = spectra.shape
    quarter = points // 4
    g, s = lax.axis_index("freq"), lax.axis_index("space")
    core, chip = lax.rem(s, 2), s // 2
    late = core if EARLY == 0 else 1 - core
    n_chips = n_space // 2
    n_y = max(n_chips // 2, 1)
    z_lo, y = chip // n_y, lax.rem(chip, n_y)
    x, z_hi = g // 2, lax.rem(g, 2)
    n_x = n_freq // 2

    def remote(src, dst, send, recv, device):
        return pltpu.make_async_remote_copy(
            src_ref=src,
            dst_ref=dst,
            send_sem=send,
            recv_sem=recv,
            device_id=device,
            device_id_type=MESH,
        )

    def space_peer(offset):
        return (g, lax.rem(s + offset, n_space))

    other_s = lax.rem(s + n_space // 2, n_space)

    def meeting(slot):
        to_x = x if slot < 2 else n_x - 1 - x
        to_z = z_hi if slot % 2 == 0 else 1 - z_hi
        part = 2 * to_z + (2 * to_x) // n_x
        return (2 * to_x + to_z, other_s), part

    def chip_ahead(ahead):
        to_z = lax.rem(z_lo + ahead // n_y, 2)
        to_y = lax.rem(y + lax.rem(ahead, n_y), n_y)
        return to_z * n_y + to_y

    def chip_at(k):
        return chip_ahead(n_chips - 1 - k)

    def place_at(step):
        step = jnp.int32(step)
        last = step == 2 * n_chips - 1
        early = step < n_chips - 1
        own_first = jnp.logical_or(early, last)
        k_first = jnp.where(early, step, jnp.where(last, n_chips - 1, step - (n_chips - 1)))
        own_last = step >= n_chips
        own = jnp.where(late == 0, own_first.astype(jnp.int32), own_last.astype(jnp.int32))
        return own, jnp.where(late == 0, k_first, lax.rem(step, n_chips))

    def slot_at(step):
        own, k = place_at(step)
        return own * n_chips + k

    def freq_at(step):
        own, k = place_at(step)
        return 2 * chip_at(k) + jnp.where(own == 1, core, 1 - core)

    def load(step):
        freq = freq_at(step)
        return pltpu.make_async_copy(spectra_hbm.at[freq], spectra.at[freq], load_sem.at[freq])

    for step in range(min(AHEAD, freqs)):
        load(step).start()

    barrier = pltpu.get_barrier_semaphore()
    for offset in range(1, n_space):
        pl.semaphore_signal(barrier, inc=1, device_id=space_peer(offset), device_id_type=MESH)
    for slot in range(1, 4):
        pl.semaphore_signal(barrier, inc=1, device_id=meeting(slot)[0], device_id_type=MESH)

    for tile in range(points // 128):
        weight_row[:, tile * 128 : (tile + 1) * 128] = weight_ref[tile : tile + 1, :]
    lanes = partner_row.shape[1]
    which = lax.broadcasted_iota(jnp.int32, (1, lanes), 1) // (2 * KMAX)
    row = jnp.zeros((1, lanes), jnp.float32)
    for freq in range(freqs):
        row = jnp.where(which == freq, partner_ref[freq].astype(jnp.float32), row)
    partner_row[...] = row

    def core_copy(step):
        return remote(
            squares.at[step],
            from_core.at[step],
            core_send.at[step],
            core_recv.at[step],
            (g, s + 1 - 2 * core),
        )

    def chip_copy(step):
        return remote(
            squares.at[n_chips + step],
            from_chips.at[step],
            chip_send.at[step],
            chip_recv.at[step],
            (g, 2 * chip_at(step) + core),
        )

    def gram(*steps):
        for step in steps:
            load(step).wait()

            @pl.when(step + AHEAD < freqs)
            def _():
                load(step + AHEAD).start()

        for step in steps:
            squares[slot_at(step)] = packed(moment(spectra[freq_at(step)], weight_row[...]))

    def hand_over(step):
        own, k = place_at(step)

        @pl.when(own == 0)
        def _():
            core_copy(k).start()

    def add_and_send(step):
        own, k = place_at(step)

        @pl.when(own == 1)
        def _():
            core_copy(k).wait_recv()
            squares[n_chips + k] = squares[n_chips + k] + from_core[k]
            chip_copy(k).start()

    gram(0, 1)
    pl.semaphore_wait(barrier, n_space - 1 + 3)
    hand_over(0)
    hand_over(1)

    @pl.loop(1, n_chips - 1)
    def _(pair):
        gram(2 * pair, 2 * pair + 1)
        hand_over(2 * pair)
        hand_over(2 * pair + 1)
        add_and_send(2 * pair - 2 + late)
        add_and_send(2 * pair - 1 + late)

    gram(2 * n_chips - 2)
    hand_over(2 * n_chips - 2)
    add_and_send(2 * n_chips - 4 + late)
    add_and_send(2 * n_chips - 3 + late)

    start = pl.multiple_of(meeting(0)[1] * quarter, 128)
    weight_copy = remote(
        weight_row.at[:, pl.ds(start, quarter)],
        weight_in,
        weight_sem.at[0],
        weight_sem.at[1],
        meeting(0)[0],
    )
    row_copies = [
        remote(
            partner_row, partner_in.at[slot], row_send.at[slot], row_recv.at[slot], meeting(slot)[0]
        )
        for slot in range(4)
    ]
    weight_copy.start()
    for copy in row_copies:
        copy.start()

    gram(2 * n_chips - 1)
    core_copy(n_chips - 1).wait_recv()
    square = squares[2 * n_chips - 1] + from_core[n_chips - 1]
    for step in range(n_chips - 1):
        chip_copy(step).wait_recv()
        square = square + from_chips[step]
    coefficient, energy = solved(*unpacked(square, total), counts_ref[s])
    coef_own[...] = coefficient
    coefs[s] = coefficient
    ranks = lax.broadcasted_iota(jnp.int32, (KMAX, 128), 0)
    lane = lax.broadcasted_iota(jnp.int32, (KMAX, 128), 1)
    energy = jnp.sum(jnp.where(ranks == lane, energy, 0.0), axis=0, keepdims=True)
    energy_own[...] = energy
    energies[s] = energy

    near = [ahead for ahead in (0, 1, 3, 4, 2, 5, 7, 6) if ahead < n_chips]

    def near_freq(place, parity):
        ahead = jnp.int32(near[0])
        for spot in range(1, n_chips):
            ahead = jnp.where(place == spot, near[spot], ahead)
        return 2 * chip_ahead(ahead) + parity

    peers = []
    for item in range(n_space - 1):
        first = item < n_chips - 1 + late
        place = jnp.where(first, item + 1 - late, item - (n_chips - 1))
        peers.append(near_freq(place, jnp.where(first, EARLY, 1 - EARLY)))

    def coef_copy(peer, owner):
        send, recv = coef_send.at[peer], coef_recv.at[owner]
        return remote(coef_own, coefs.at[owner], send, recv, (g, peer))

    coef_copies, energy_copies, sum_copies = [], [], []
    for peer in peers:
        coef_copies.append(coef_copy(peer, s))
        send, recv = energy_send.at[peer], energy_recv.at[s]
        energy_copies.append(remote(energy_own, energies.at[s], send, recv, (g, peer)))
        send, recv = sum_send.at[peer], sum_recv.at[s]
        sum_copies.append(remote(sums.at[s], sums.at[s], send, recv, (g, peer)))
    for copy in coef_copies:
        copy.start()
    for copy in energy_copies:
        copy.start()

    def mode_copy(freq, slot):
        device, part = meeting(slot)
        start = pl.multiple_of(part * quarter, 128)
        return remote(
            modes.at[freq, :, pl.ds(start, quarter)],
            arrived.at[slot, freq],
            mode_send.at[slot, freq],
            mode_recv.at[slot, freq],
            device,
        )

    def mode_store(freq):
        return pltpu.make_async_copy(modes.at[freq], modes_hbm.at[freq], store_sem.at[freq])

    @pl.loop(0, freqs)
    def _(step):
        first = step < n_chips + late
        place = jnp.where(step == 0, 0, jnp.where(first, step - late, step - n_chips))
        parity = jnp.where(step == 0, core, jnp.where(first, EARLY, 1 - EARLY))
        freq = near_freq(place, parity)

        @pl.when(step > 0)
        def _():
            coef_copy(freq, freq).wait_recv()

        modes[freq] = times_transposed(both_halves(coefs[freq]), spectra[freq]).astype(jnp.bfloat16)
        for slot in (2, 3, 0, 1):
            mode_copy(freq, slot).start()
        mode_store(freq).start()

    for copy in row_copies:
        copy.wait_recv()
    weight_copy.wait_recv()

    @pl.loop(0, freqs)
    def _(freq):
        for slot in range(4):
            mode_copy(freq, slot).wait_recv()

    rows = 2 * KMAX * freqs
    owner = lax.broadcasted_iota(jnp.int32, (rows, rows), 0) // (2 * KMAX)
    owner = owner.astype(jnp.float32)
    is_re = lax.rem(lax.broadcasted_iota(jnp.int32, (KMAX, rows), 1), 2 * KMAX) < KMAX
    line = weight_in[...]
    part_copies = []
    for slot in (2, 3, 0, 1):
        phi = arrived[slot].reshape(rows, quarter)
        psi = arrived[3 - slot].reshape(rows, quarter)
        wpsi = (psi.astype(jnp.float32) * line).astype(jnp.bfloat16)
        cross = times_transposed(wpsi, phi)
        cross = jnp.where(owner == partner_in[slot], cross, 0.0)
        chosen = jnp.sum(cross.reshape(freqs, 2 * KMAX, rows), axis=0)
        low, high = chosen[:KMAX], chosen[KMAX:]
        parts[slot] = jnp.where(
            is_re,
            low + pltpu.roll(high, rows - KMAX, 1),
            pltpu.roll(high, KMAX, 1) - low,
        )
        copy = remote(
            parts.at[slot],
            parts_in.at[slot],
            part_send.at[slot],
            part_recv.at[slot],
            meeting(slot)[0],
        )
        copy.start()
        part_copies.append(copy)
    for copy in part_copies:
        copy.wait_recv()
    sums[s] = (parts_in[0] + parts_in[1]) + (parts_in[2] + parts_in[3])
    for copy in sum_copies:
        copy.start()
    for peer in peers:
        send, recv = energy_send.at[peer], energy_recv.at[peer]
        remote(energy_own, energies.at[peer], send, recv, (g, peer)).wait_recv()
    gathered = jnp.concatenate([energies[k] for k in range(freqs)], axis=0)
    energy_ref[...] = gathered.T[:KMAX]

    for peer in peers:
        send, recv = sum_send.at[peer], sum_recv.at[peer]
        remote(sums.at[s], sums.at[peer], send, recv, (g, peer)).wait_recv()
    whole = sums[0]
    for place in range(1, n_space):
        whole = whole + sums[place]
    coherence_ref[...] = whole / total

    @pl.loop(0, n_chips)
    def _(step):
        core_copy(step).wait_send()

    @pl.loop(0, n_chips - 1)
    def _(step):
        chip_copy(step).wait_send()

    @pl.loop(0, freqs)
    def _(freq):
        for slot in range(4):
            mode_copy(freq, slot).wait_send()
        mode_store(freq).wait()

    sends = row_copies + coef_copies + energy_copies + part_copies + sum_copies
    for copy in [weight_copy] + sends:
        copy.wait_send()


def with_freq_last(value, freqs):
    lanes, both = value.shape[1], 2 * KMAX
    old = lax.broadcasted_iota(jnp.int32, (lanes, lanes), 0)
    new = lax.broadcasted_iota(jnp.int32, (lanes, lanes), 1)
    moves = jnp.logical_and(old // both == lax.rem(new, freqs), lax.rem(old, both) == new // freqs)
    moves = jnp.where(moves, 1.0, 0.0).astype(jnp.bfloat16)
    high = value.astype(jnp.bfloat16).astype(jnp.float32)
    mid = (value - high).astype(jnp.bfloat16).astype(jnp.float32)
    pieces = jnp.concatenate([high, mid, value - high - mid, jnp.zeros_like(value)], axis=0)
    moved = jnp.dot(pieces.astype(jnp.bfloat16), moves, preferred_element_type=jnp.float32)
    return moved[:KMAX] + (moved[KMAX:both] + moved[both : both + KMAX])


def hand_on(modes_in, energy_in, coherence_in, modes_out, energy_out, coherence_out, *scratch):
    modes, energy, coherence, spread, ins, outs = scratch
    freqs = modes.shape[0]

    def taken(freq):
        return pltpu.make_async_copy(modes_in.at[freq], modes.at[freq], ins.at[freq])

    def given(freq):
        return pltpu.make_async_copy(modes.at[freq], modes_out.at[freq], outs.at[freq])

    small_in = [
        pltpu.make_async_copy(coherence_in, coherence, ins.at[freqs]),
        pltpu.make_async_copy(energy_in, energy, ins.at[freqs + 1]),
    ]
    small_out = [
        pltpu.make_async_copy(spread, coherence_out, outs.at[freqs]),
        pltpu.make_async_copy(energy, energy_out, outs.at[freqs + 1]),
    ]
    for copy in small_in:
        copy.start()
    for freq in range(freqs):
        taken(freq).start()
    for copy in small_in:
        copy.wait()
    small_out[1].start()
    moved = with_freq_last(coherence[...], freqs)
    for place in range(2 * KMAX):
        piece = moved[:, place * freqs : (place + 1) * freqs]
        spread[place // KMAX, place % KMAX] = piece
    for freq in range(freqs):
        taken(freq).wait()
        given(freq).start()
    small_out[0].start()
    for freq in range(freqs):
        given(freq).wait()
    for copy in small_out:
        copy.wait()


def on_device(n_freq, n_space, spectra, weight, partner, counts):
    freqs, points, wide = spectra.shape
    half = wide // 2
    rows = 2 * KMAX
    lanes = rows * freqs
    quarter = points // 4
    n_chips = n_space // 2
    f32, bf16 = jnp.float32, jnp.bfloat16
    dma = pltpu.SemaphoreType.DMA
    vmem, smem = pltpu.VMEM, pltpu.SMEM
    modes, energy, coherence = pl.pallas_call(
        functools.partial(kernel, n_freq, n_space, points * n_space),
        out_shape=(
            jax.ShapeDtypeStruct((freqs, rows, points), bf16),
            jax.ShapeDtypeStruct((KMAX, freqs), f32),
            jax.ShapeDtypeStruct((KMAX, lanes), f32),
        ),
        in_specs=[
            pl.BlockSpec(memory_space=pl.ANY),
            pl.BlockSpec(memory_space=vmem),
            pl.BlockSpec(memory_space=smem),
            pl.BlockSpec(memory_space=smem),
        ],
        out_specs=(
            pl.BlockSpec(memory_space=pltpu.HBM),
            pl.BlockSpec(memory_space=vmem),
            pl.BlockSpec(memory_space=vmem),
        ),
        scratch_shapes=[
            vmem((freqs, points, wide), bf16),
            vmem((2 * n_chips, half, half), f32),
            vmem((n_chips, half, half), f32),
            vmem((n_chips, half, half), f32),
            vmem((KMAX, wide), bf16),
            vmem((freqs, KMAX, wide), bf16),
            vmem((1, 128), f32),
            vmem((freqs, 1, 128), f32),
            vmem((freqs, rows, points), bf16),
            vmem((4, freqs, rows, quarter), bf16),
            vmem((1, points), f32),
            vmem((1, quarter), f32),
            vmem((1, lanes), f32),
            vmem((4, 1, lanes), f32),
            vmem((4, KMAX, lanes), f32),
            vmem((4, KMAX, lanes), f32),
            vmem((n_space, KMAX, lanes), f32),
            dma((freqs,)),
            dma((freqs,)),
            dma((n_chips,)),
            dma((n_chips,)),
            dma((n_chips,)),
            dma((n_chips,)),
            dma((n_space,)),
            dma((n_space,)),
            dma((n_space,)),
            dma((n_space,)),
            dma((4, freqs)),
            dma((4, freqs)),
            dma((2,)),
            dma((4,)),
            dma((4,)),
            dma((4,)),
            dma((4,)),
            dma((n_space,)),
            dma((n_space,)),
        ],
        compiler_params=pltpu.CompilerParams(
            collective_id=0, has_side_effects=True, vmem_limit_bytes=60 * 1024 * 1024
        ),
    )(spectra, weight.reshape(points // 128, 128), partner, counts)
    last = jax.ShapeDtypeStruct((2, KMAX, KMAX, freqs), f32)
    modes, energy, coherence = pl.pallas_call(
        hand_on,
        out_shape=(
            jax.ShapeDtypeStruct(modes.shape, bf16),
            jax.ShapeDtypeStruct(energy.shape, f32),
            last,
        ),
        in_specs=[pl.BlockSpec(memory_space=pltpu.HBM)] * 3,
        out_specs=(pl.BlockSpec(memory_space=pltpu.HBM),) * 3,
        scratch_shapes=[
            vmem(modes.shape, bf16),
            vmem(energy.shape, f32),
            vmem(coherence.shape, f32),
            vmem(last.shape, f32),
            dma((freqs + 2,)),
            dma((freqs + 2,)),
        ],
    )(modes, energy, coherence)
    return modes, energy.T, coherence.transpose(3, 0, 1, 2)


def solution(mesh):
    in_specs = (P("freq", "space", None), P("space"), P("freq"), P("freq"))
    out_specs = (P("freq", None, "space"), P("freq", None), P("freq", None, None, None))
    body = functools.partial(on_device, mesh.shape["freq"], mesh.shape["space"])
    return jax.shard_map(
        body, mesh=mesh, in_specs=in_specs, out_specs=out_specs, check_vma=False
    )
```

```python
import functools

import jax
import jax.numpy as jnp
from jax import lax
from jax.experimental import pallas as pl
from jax.experimental.pallas import tpu as pltpu
from jax.sharding import PartitionSpec as P

KMAX = 8
ITERS = 4
EPS = 1e-06
AHEAD = 5
EARLY = 1
MESH = pl.DeviceIdType.MESH
HIGHEST = lax.Precision.HIGHEST


def moment(spectra, weight):
    turned = spectra.T.astype(jnp.float32) * weight
    return jnp.dot(turned.astype(jnp.bfloat16), spectra, preferred_element_type=jnp.float32)


def times_transposed(left, right):
    return lax.dot_general(
        left, right, (((1,), (1,)), ((), ())), preferred_element_type=jnp.float32
    )


def triangles(half):
    row = lax.broadcasted_iota(jnp.int32, (half, half), 0)
    col = lax.broadcasted_iota(jnp.int32, (half, half), 1)
    return row, col


def packed(moments):
    half = moments.shape[0] // 2
    row, col = triangles(half)
    gram_re = moments[:half, :half] + moments[half:, half:]
    gram_im = moments[:half, half:] - moments[half:, :half]
    return jnp.where(row <= col, gram_re, gram_im)


def unpacked(square, total):
    row, col = triangles(square.shape[0])
    flipped = square.T
    gram_re = jnp.where(row <= col, square, flipped)
    gram_im = jnp.where(row > col, square, jnp.where(row < col, -flipped, 0.0))
    return gram_re / total, gram_im / total


def orthonormal(vec_re, vec_im):
    ranks = lax.broadcasted_iota(jnp.int32, vec_re.shape, 0)
    for k in range(KMAX):
        own_re = jnp.broadcast_to(vec_re[k : k + 1], vec_re.shape)
        own_im = jnp.broadcast_to(vec_im[k : k + 1], vec_im.shape)
        norm = jnp.sum(own_re * own_re + own_im * own_im, axis=1, keepdims=True)
        proj_re = jnp.sum(own_re * vec_re + own_im * vec_im, axis=1, keepdims=True)
        proj_im = jnp.sum(own_re * vec_im - own_im * vec_re, axis=1, keepdims=True)
        inverse = lax.rsqrt(norm + EPS)
        unit_re, unit_im = own_re * inverse, own_im * inverse
        proj_re, proj_im = proj_re * inverse, proj_im * inverse
        new_re = vec_re - proj_re * unit_re + proj_im * unit_im
        new_im = vec_im - proj_re * unit_im - proj_im * unit_re
        vec_re = jnp.where(ranks > k, new_re, jnp.where(ranks == k, unit_re, vec_re))
        vec_im = jnp.where(ranks > k, new_im, jnp.where(ranks == k, unit_im, vec_im))
    return vec_re, vec_im


def solved(gram_re, gram_im, count):
    half = gram_re.shape[0]
    operator = jnp.concatenate([gram_re, gram_im], axis=1)

    def applied(vec_re, vec_im):
        both = jnp.concatenate([vec_re, vec_im], axis=0)
        image = jnp.dot(both, operator, precision=HIGHEST, preferred_element_type=jnp.float32)
        return (
            image[:KMAX, :half] + image[KMAX:, half:],
            image[KMAX:, :half] - image[:KMAX, half:],
        )

    vec_re, vec_im = orthonormal(gram_re[:KMAX], -gram_im[:KMAX])
    for _ in range(ITERS - 1):
        vec_re, vec_im = orthonormal(*applied(vec_re, vec_im))
    image_re, image_im = applied(vec_re, vec_im)
    energy = jnp.sum(vec_re * image_re + vec_im * image_im, axis=1, keepdims=True)
    ranks = lax.broadcasted_iota(jnp.int32, (KMAX, 1), 0)
    scale = jnp.where(ranks < count, lax.rsqrt(energy + EPS), 0.0)
    part_re, part_im = vec_re * scale, vec_im * scale
    return jnp.concatenate([part_re, -part_im], axis=1).astype(jnp.bfloat16), energy


def both_halves(upper):
    half = upper.shape[1] // 2
    upper = upper.astype(jnp.float32)
    lower = jnp.concatenate([-upper[:, half:], upper[:, :half]], axis=1)
    return jnp.concatenate([upper, lower], axis=0).astype(jnp.bfloat16)


def kernel(
    n_freq,
    n_space,
    total,
    spectra_hbm,
    weight_ref,
    partner_ref,
    counts_ref,
    modes_hbm,
    energy_ref,
    coherence_ref,
    spectra,
    squares,
    from_core,
    from_chips,
    coef_own,
    coefs,
    energy_own,
    energies,
    modes,
    arrived,
    weight_row,
    weight_in,
    partner_row,
    partner_in,
    parts,
    parts_in,
    sums,
    load_sem,
    store_sem,
    core_send,
    core_recv,
    chip_send,
    chip_recv,
    coef_send,
    coef_recv,
    energy_send,
    energy_recv,
    mode_send,
    mode_recv,
    weight_sem,
    row_send,
    row_recv,
    part_send,
    part_recv,
    sum_send,
    sum_recv,
):
    freqs, points, wide = spectra.shape
    quarter = points // 4
    g, s = lax.axis_index("freq"), lax.axis_index("space")
    core, chip = lax.rem(s, 2), s // 2
    late = core if EARLY == 0 else 1 - core
    n_chips = n_space // 2
    n_y = max(n_chips // 2, 1)
    z_lo, y = chip // n_y, lax.rem(chip, n_y)
    x, z_hi = g // 2, lax.rem(g, 2)
    n_x = n_freq // 2

    def remote(src, dst, send, recv, device):
        return pltpu.make_async_remote_copy(
            src_ref=src,
            dst_ref=dst,
            send_sem=send,
            recv_sem=recv,
            device_id=device,
            device_id_type=MESH,
        )

    def space_peer(offset):
        return (g, lax.rem(s + offset, n_space))

    other_s = lax.rem(s + n_space // 2, n_space)

    def meeting(slot):
        to_x = x if slot < 2 else n_x - 1 - x
        to_z = z_hi if slot % 2 == 0 else 1 - z_hi
        part = 2 * to_z + (2 * to_x) // n_x
        return (2 * to_x + to_z, other_s), part

    def chip_ahead(ahead):
        to_z = lax.rem(z_lo + ahead // n_y, 2)
        to_y = lax.rem(y + lax.rem(ahead, n_y), n_y)
        return to_z * n_y + to_y

    def chip_at(k):
        return chip_ahead(n_chips - 1 - k)

    def place_at(step):
        step = jnp.int32(step)
        last = step == 2 * n_chips - 1
        early = step < n_chips - 1
        own_first = jnp.logical_or(early, last)
        k_first = jnp.where(early, step, jnp.where(last, n_chips - 1, step - (n_chips - 1)))
        own_last = step >= n_chips
        own = jnp.where(late == 0, own_first.astype(jnp.int32), own_last.astype(jnp.int32))
        return own, jnp.where(late == 0, k_first, lax.rem(step, n_chips))

    def slot_at(step):
        own, k = place_at(step)
        return own * n_chips + k

    def freq_at(step):
        own, k = place_at(step)
        return 2 * chip_at(k) + jnp.where(own == 1, core, 1 - core)

    def load(step):
        freq = freq_at(step)
        return pltpu.make_async_copy(spectra_hbm.at[freq], spectra.at[freq], load_sem.at[freq])

    for step in range(min(AHEAD, freqs)):
        load(step).start()

    barrier = pltpu.get_barrier_semaphore()
    for offset in range(1, n_space):
        pl.semaphore_signal(barrier, inc=1, device_id=space_peer(offset), device_id_type=MESH)
    for slot in range(1, 4):
        pl.semaphore_signal(barrier, inc=1, device_id=meeting(slot)[0], device_id_type=MESH)

    for tile in range(points // 128):
        weight_row[:, tile * 128 : (tile + 1) * 128] = weight_ref[tile : tile + 1, :]
    lanes = partner_row.shape[1]
    which = lax.broadcasted_iota(jnp.int32, (1, lanes), 1) // (2 * KMAX)
    row = jnp.zeros((1, lanes), jnp.float32)
    for freq in range(freqs):
        row = jnp.where(which == freq, partner_ref[freq].astype(jnp.float32), row)
    partner_row[...] = row

    def core_copy(step):
        return remote(
            squares.at[step],
            from_core.at[step],
            core_send.at[step],
            core_recv.at[step],
            (g, s + 1 - 2 * core),
        )

    def chip_copy(step):
        return remote(
            squares.at[n_chips + step],
            from_chips.at[step],
            chip_send.at[step],
            chip_recv.at[step],
            (g, 2 * chip_at(step) + core),
        )

    def gram(*steps):
        for step in steps:
            load(step).wait()

            @pl.when(step + AHEAD < freqs)
            def _():
                load(step + AHEAD).start()

        for step in steps:
            squares[slot_at(step)] = packed(moment(spectra[freq_at(step)], weight_row[...]))

    def hand_over(step):
        own, k = place_at(step)

        @pl.when(own == 0)
        def _():
            core_copy(k).start()

    def add_and_send(step):
        own, k = place_at(step)

        @pl.when(own == 1)
        def _():
            core_copy(k).wait_recv()
            squares[n_chips + k] = squares[n_chips + k] + from_core[k]
            chip_copy(k).start()

    gram(0, 1)
    pl.semaphore_wait(barrier, n_space - 1 + 3)
    hand_over(0)
    hand_over(1)

    @pl.loop(1, n_chips - 1)
    def _(pair):
        gram(2 * pair, 2 * pair + 1)
        hand_over(2 * pair)
        hand_over(2 * pair + 1)
        add_and_send(2 * pair - 2 + late)
        add_and_send(2 * pair - 1 + late)

    gram(2 * n_chips - 2, 2 * n_chips - 1)
    hand_over(2 * n_chips - 2)
    add_and_send(2 * n_chips - 4 + late)
    add_and_send(2 * n_chips - 3 + late)

    start = pl.multiple_of(meeting(0)[1] * quarter, 128)
    weight_copy = remote(
        weight_row.at[:, pl.ds(start, quarter)],
        weight_in,
        weight_sem.at[0],
        weight_sem.at[1],
        meeting(0)[0],
    )
    row_copies = [
        remote(
            partner_row, partner_in.at[slot], row_send.at[slot], row_recv.at[slot], meeting(slot)[0]
        )
        for slot in range(4)
    ]
    weight_copy.start()
    for copy in row_copies:
        copy.start()

    core_copy(n_chips - 1).wait_recv()
    square = squares[2 * n_chips - 1] + from_core[n_chips - 1]
    for step in range(n_chips - 1):
        chip_copy(step).wait_recv()
        square = square + from_chips[step]
    coefficient, energy = solved(*unpacked(square, total), counts_ref[s])
    coef_own[...] = coefficient
    coefs[s] = coefficient
    ranks = lax.broadcasted_iota(jnp.int32, (KMAX, 128), 0)
    lane = lax.broadcasted_iota(jnp.int32, (KMAX, 128), 1)
    energy = jnp.sum(jnp.where(ranks == lane, energy, 0.0), axis=0, keepdims=True)
    energy_own[...] = energy
    energies[s] = energy

    near = [ahead for ahead in (0, 1, 3, 4, 2, 5, 7, 6) if ahead < n_chips]

    def near_freq(place, parity):
        ahead = jnp.int32(near[0])
        for spot in range(1, n_chips):
            ahead = jnp.where(place == spot, near[spot], ahead)
        return 2 * chip_ahead(ahead) + parity

    peers = []
    for item in range(n_space - 1):
        first = item < n_chips - 1 + late
        place = jnp.where(first, item + 1 - late, item - (n_chips - 1))
        peers.append(near_freq(place, jnp.where(first, EARLY, 1 - EARLY)))

    def coef_copy(peer, owner):
        send, recv = coef_send.at[peer], coef_recv.at[owner]
        return remote(coef_own, coefs.at[owner], send, recv, (g, peer))

    coef_copies, energy_copies, sum_copies = [], [], []
    for peer in peers:
        coef_copies.append(coef_copy(peer, s))
        send, recv = energy_send.at[peer], energy_recv.at[s]
        energy_copies.append(remote(energy_own, energies.at[s], send, recv, (g, peer)))
        send, recv = sum_send.at[peer], sum_recv.at[s]
        sum_copies.append(remote(sums.at[s], sums.at[s], send, recv, (g, peer)))
    for copy in coef_copies:
        copy.start()
    for copy in energy_copies:
        copy.start()

    def mode_copy(freq, slot):
        device, part = meeting(slot)
        start = pl.multiple_of(part * quarter, 128)
        return remote(
            modes.at[freq, :, pl.ds(start, quarter)],
            arrived.at[slot, freq],
            mode_send.at[slot, freq],
            mode_recv.at[slot, freq],
            device,
        )

    def mode_store(freq):
        return pltpu.make_async_copy(modes.at[freq], modes_hbm.at[freq], store_sem.at[freq])

    @pl.loop(0, freqs)
    def _(step):
        first = step < n_chips + late
        place = jnp.where(step == 0, 0, jnp.where(first, step - late, step - n_chips))
        parity = jnp.where(step == 0, core, jnp.where(first, EARLY, 1 - EARLY))
        freq = near_freq(place, parity)

        @pl.when(step > 0)
        def _():
            coef_copy(freq, freq).wait_recv()

        modes[freq] = times_transposed(both_halves(coefs[freq]), spectra[freq]).astype(jnp.bfloat16)
        for slot in (2, 3, 0, 1):
            mode_copy(freq, slot).start()
        mode_store(freq).start()

    for copy in row_copies:
        copy.wait_recv()
    weight_copy.wait_recv()

    @pl.loop(0, freqs)
    def _(freq):
        for slot in range(4):
            mode_copy(freq, slot).wait_recv()

    rows = 2 * KMAX * freqs
    owner = lax.broadcasted_iota(jnp.int32, (rows, rows), 0) // (2 * KMAX)
    owner = owner.astype(jnp.float32)
    is_re = lax.rem(lax.broadcasted_iota(jnp.int32, (KMAX, rows), 1), 2 * KMAX) < KMAX
    line = weight_in[...]
    part_copies = []
    for slot in (2, 3, 0, 1):
        phi = arrived[slot].reshape(rows, quarter)
        psi = arrived[3 - slot].reshape(rows, quarter)
        wpsi = (psi.astype(jnp.float32) * line).astype(jnp.bfloat16)
        cross = times_transposed(wpsi, phi)
        cross = jnp.where(owner == partner_in[slot], cross, 0.0)
        chosen = jnp.sum(cross.reshape(freqs, 2 * KMAX, rows), axis=0)
        low, high = chosen[:KMAX], chosen[KMAX:]
        parts[slot] = jnp.where(
            is_re,
            low + pltpu.roll(high, rows - KMAX, 1),
            pltpu.roll(high, KMAX, 1) - low,
        )
        copy = remote(
            parts.at[slot],
            parts_in.at[slot],
            part_send.at[slot],
            part_recv.at[slot],
            meeting(slot)[0],
        )
        copy.start()
        part_copies.append(copy)
    for copy in part_copies:
        copy.wait_recv()
    sums[s] = (parts_in[0] + parts_in[1]) + (parts_in[2] + parts_in[3])
    for copy in sum_copies:
        copy.start()
    for peer in peers:
        send, recv = energy_send.at[peer], energy_recv.at[peer]
        remote(energy_own, energies.at[peer], send, recv, (g, peer)).wait_recv()
    gathered = jnp.concatenate([energies[k] for k in range(freqs)], axis=0)
    energy_ref[...] = gathered.T[:KMAX]

    for peer in peers:
        send, recv = sum_send.at[peer], sum_recv.at[peer]
        remote(sums.at[s], sums.at[peer], send, recv, (g, peer)).wait_recv()
    whole = sums[0]
    for place in range(1, n_space):
        whole = whole + sums[place]
    coherence_ref[...] = whole / total

    @pl.loop(0, n_chips)
    def _(step):
        core_copy(step).wait_send()

    @pl.loop(0, n_chips - 1)
    def _(step):
        chip_copy(step).wait_send()

    @pl.loop(0, freqs)
    def _(freq):
        for slot in range(4):
            mode_copy(freq, slot).wait_send()
        mode_store(freq).wait()

    sends = row_copies + coef_copies + energy_copies + part_copies + sum_copies
    for copy in [weight_copy] + sends:
        copy.wait_send()


def with_freq_last(value, freqs):
    lanes, both = value.shape[1], 2 * KMAX
    old = lax.broadcasted_iota(jnp.int32, (lanes, lanes), 0)
    new = lax.broadcasted_iota(jnp.int32, (lanes, lanes), 1)
    moves = jnp.logical_and(old // both == lax.rem(new, freqs), lax.rem(old, both) == new // freqs)
    moves = jnp.where(moves, 1.0, 0.0).astype(jnp.bfloat16)
    high = value.astype(jnp.bfloat16).astype(jnp.float32)
    mid = (value - high).astype(jnp.bfloat16).astype(jnp.float32)
    pieces = jnp.concatenate([high, mid, value - high - mid, jnp.zeros_like(value)], axis=0)
    moved = jnp.dot(pieces.astype(jnp.bfloat16), moves, preferred_element_type=jnp.float32)
    return moved[:KMAX] + (moved[KMAX:both] + moved[both : both + KMAX])


def hand_on(modes_in, energy_in, coherence_in, modes_out, energy_out, coherence_out, *scratch):
    modes, energy, coherence, spread, ins, outs = scratch
    freqs = modes.shape[0]
    many = freqs // 4

    def taken(part):
        rows = pl.ds(part * many, many)
        return pltpu.make_async_copy(modes_in.at[rows], modes.at[rows], ins.at[part])

    def given(part):
        rows = pl.ds(part * many, many)
        return pltpu.make_async_copy(modes.at[rows], modes_out.at[rows], outs.at[part])

    small_in = [
        pltpu.make_async_copy(coherence_in, coherence, ins.at[freqs]),
        pltpu.make_async_copy(energy_in, energy, ins.at[freqs + 1]),
    ]
    small_out = [
        pltpu.make_async_copy(spread, coherence_out, outs.at[freqs]),
        pltpu.make_async_copy(energy, energy_out, outs.at[freqs + 1]),
    ]
    for copy in small_in:
        copy.start()
    for part in range(4):
        taken(part).start()
    for copy in small_in:
        copy.wait()
    small_out[1].start()
    moved = with_freq_last(coherence[...], freqs)
    for place in range(2 * KMAX):
        piece = moved[:, place * freqs : (place + 1) * freqs]
        spread[place // KMAX, place % KMAX] = piece
    for part in range(4):
        taken(part).wait()
        given(part).start()
    small_out[0].start()
    for part in range(4):
        given(part).wait()
    for copy in small_out:
        copy.wait()


def on_device(n_freq, n_space, spectra, weight, partner, counts):
    freqs, points, wide = spectra.shape
    half = wide // 2
    rows = 2 * KMAX
    lanes = rows * freqs
    quarter = points // 4
    n_chips = n_space // 2
    f32, bf16 = jnp.float32, jnp.bfloat16
    dma = pltpu.SemaphoreType.DMA
    vmem, smem = pltpu.VMEM, pltpu.SMEM
    modes, energy, coherence = pl.pallas_call(
        functools.partial(kernel, n_freq, n_space, points * n_space),
        out_shape=(
            jax.ShapeDtypeStruct((freqs, rows, points), bf16),
            jax.ShapeDtypeStruct((KMAX, freqs), f32),
            jax.ShapeDtypeStruct((KMAX, lanes), f32),
        ),
        in_specs=[
            pl.BlockSpec(memory_space=pl.ANY),
            pl.BlockSpec(memory_space=vmem),
            pl.BlockSpec(memory_space=smem),
            pl.BlockSpec(memory_space=smem),
        ],
        out_specs=(
            pl.BlockSpec(memory_space=pltpu.HBM),
            pl.BlockSpec(memory_space=vmem),
            pl.BlockSpec(memory_space=vmem),
        ),
        scratch_shapes=[
            vmem((freqs, points, wide), bf16),
            vmem((2 * n_chips, half, half), f32),
            vmem((n_chips, half, half), f32),
            vmem((n_chips, half, half), f32),
            vmem((KMAX, wide), bf16),
            vmem((freqs, KMAX, wide), bf16),
            vmem((1, 128), f32),
            vmem((freqs, 1, 128), f32),
            vmem((freqs, rows, points), bf16),
            vmem((4, freqs, rows, quarter), bf16),
            vmem((1, points), f32),
            vmem((1, quarter), f32),
            vmem((1, lanes), f32),
            vmem((4, 1, lanes), f32),
            vmem((4, KMAX, lanes), f32),
            vmem((4, KMAX, lanes), f32),
            vmem((n_space, KMAX, lanes), f32),
            dma((freqs,)),
            dma((freqs,)),
            dma((n_chips,)),
            dma((n_chips,)),
            dma((n_chips,)),
            dma((n_chips,)),
            dma((n_space,)),
            dma((n_space,)),
            dma((n_space,)),
            dma((n_space,)),
            dma((4, freqs)),
            dma((4, freqs)),
            dma((2,)),
            dma((4,)),
            dma((4,)),
            dma((4,)),
            dma((4,)),
            dma((n_space,)),
            dma((n_space,)),
        ],
        compiler_params=pltpu.CompilerParams(
            collective_id=0, has_side_effects=True, vmem_limit_bytes=60 * 1024 * 1024
        ),
    )(spectra, weight.reshape(points // 128, 128), partner, counts)
    last = jax.ShapeDtypeStruct((2, KMAX, KMAX, freqs), f32)
    modes, energy, coherence = pl.pallas_call(
        hand_on,
        out_shape=(
            jax.ShapeDtypeStruct(modes.shape, bf16),
            jax.ShapeDtypeStruct(energy.shape, f32),
            last,
        ),
        in_specs=[pl.BlockSpec(memory_space=pltpu.HBM)] * 3,
        out_specs=(pl.BlockSpec(memory_space=pltpu.HBM),) * 3,
        scratch_shapes=[
            vmem(modes.shape, bf16),
            vmem(energy.shape, f32),
            vmem(coherence.shape, f32),
            vmem(last.shape, f32),
            dma((freqs + 2,)),
            dma((freqs + 2,)),
        ],
    )(modes, energy, coherence)
    return modes, energy.T, coherence.transpose(3, 0, 1, 2)


def solution(mesh):
    in_specs = (P("freq", "space", None), P("space"), P("freq"), P("freq"))
    out_specs = (P("freq", None, "space"), P("freq", None), P("freq", None, None, None))
    body = functools.partial(on_device, mesh.shape["freq"], mesh.shape["space"])
    return jax.shard_map(
        body, mesh=mesh, in_specs=in_specs, out_specs=out_specs, check_vma=False
    )
```
